32 devices in a mesh: slot: 2 (over x), region: 16 (over z, y, core).
Axes of the slice: x: 2, y: 2, z: 4, core: 2. Of those that a mesh axis runs over, the one named last changes fastest.
Arguments:
- ensemble: bfloat16 [4, 128, 512, 128], P('slot', 'region'), may hold values from -6 to 6
- observations: float32 [4, 128, 1024], P('slot', 'region'), may hold values from -12 to 12
- operator_weight: bfloat16 [1024, 512], replicated, may hold values from -0.25 to 0.25
- obs_precision: float32 [1024], replicated, may hold values from 0.02 to 0.2
- channel_mask: int32 [4, 1024], P('slot'), may hold values 0 or 1
Outputs:
- analysis: bfloat16 [4, 128, 512, 128], P('slot', 'region')
The draws below stay inside these ranges and needn't reach their ends.
All inputs are finite; a program needn't handle non-finite values. No bound on the sum of `channel_mask` on one device may be relied on, other than what follows from the above.
Results may differ from the reference program's by a relative error of at most 0.014.
Values may be sent and summed in bfloat16 or wider, within the bound.
No kernel may reach another device: no remote copies, remote signals or barrier semaphores. Data moves between devices by JAX's collectives and lax.ppermute only.
A program may use at most 64 MiB of HBM per device.

```python
import math
import jax
import jax.numpy as jnp
from jax import lax

M = 128
CH = 1024
ROWS = 512
OUTER = 2
NS_STEPS = 8
SLOTS = 4
PATCHES = 128


def draw_ensemble(key, part):
    subspace = max(M // 4, 4)
    subkeys = jax.random.split(jax.random.fold_in(key, 11), 5)
    patterns = jax.random.normal(subkeys[0], (PATCHES, subspace, M), jnp.float32)
    loadings = jax.random.normal(subkeys[1], (SLOTS, PATCHES, ROWS, subspace), jnp.float32)
    noise_part = 0.35 * jax.random.normal(subkeys[3], (SLOTS, PATCHES, ROWS, M), jnp.float32)
    offset = 0.5 * jax.random.normal(subkeys[4], (SLOTS, PATCHES, ROWS, 1), jnp.float32)
    combined = jnp.einsum('tprk,pkm->tprm', loadings, patterns) * (0.9 / math.sqrt(subspace))
    values = combined + noise_part + offset
    return jnp.clip(values, -6.0, 6.0).astype(jnp.bfloat16)


def with_ends(drawn, key, low, high):
    longest = drawn.shape.index(max(drawn.shape))
    spots = []
    for shift in (0, 1):
        where = [jax.random.randint(jax.random.fold_in(key, axis), (), 0, length) for axis, length in enumerate(drawn.shape)]
        where[longest] = (where[longest] + shift) % drawn.shape[longest]
        spots.append(tuple(where))
    return drawn.at[spots[0]].set(low).at[spots[1]].set(high)


def steps_of(stream_key, shape, shards, least, high):
    def one(position, shards_of):
        heights = jax.random.uniform(jax.random.fold_in(jax.random.fold_in(stream_key, 6), position), (shards_of,), jnp.float32, least / len(shards), high / len(shards))
        return jnp.repeat(jnp.exp(heights), shape[position] // shards_of).reshape((-1,) + (1,) * (len(shape) - position - 1))

    loudness = one(*shards[0])
    for cut in shards[1:]:
        loudness = loudness * one(*cut)
    return loudness


def centred(rng, dims, scale, limit, cuts=(), kind=jnp.bfloat16):
    level = steps_of(rng, dims, cuts, -0.22, 0.18) if cuts else 1.0
    result = jax.random.normal(rng, dims, jnp.float32) * scale * level
    return jnp.minimum(jnp.maximum(result, -limit), limit).astype(kind)


def setup_inputs(seed: int = 0) -> dict:
    keys = jax.random.split(jax.random.key(seed), 6)
    ensemble = draw_ensemble(jax.random.fold_in(keys[5], 71), 0)
    observations = centred(keys[1], (SLOTS, PATCHES, CH), 2.0, 12.0, ((0, 2), (1, 16)), jnp.float32)
    operator_weight = centred(keys[2], (CH, ROWS), ROWS ** -0.5, 0.25)
    obs_precision = jnp.clip(jnp.exp(jax.random.uniform(keys[3], (CH,), jnp.float32, math.log(0.02), math.log(0.2))), 0.02, 0.2)
    channel_mask = with_ends((jax.random.randint(keys[4], (SLOTS, CH), 0, 4) < 3).astype(jnp.int32), jax.random.fold_in(keys[4], 1), 0, 1)
    return dict(ensemble=ensemble, observations=observations, operator_weight=operator_weight, obs_precision=obs_precision, channel_mask=channel_mask)


LOCAL_WEIGHT = 0.5

def quad_terms(misfit, weights):
    member_mean = lax.optimization_barrier(jnp.mean(misfit.astype(jnp.float32), axis=-1))
    spread = (misfit.astype(jnp.float32) - member_mean[..., None]).astype(jnp.bfloat16)
    weighted = (weights[:, :, None] * spread.astype(jnp.float32)).astype(jnp.bfloat16)
    innovation = (-weights * member_mean).astype(jnp.bfloat16)
    gram_part = jnp.einsum('tcm,tcn->mn', weighted.astype(jnp.float32), spread.astype(jnp.float32), precision=lax.Precision.HIGHEST)
    grad_part = jnp.einsum('tcm,tc->m', spread.astype(jnp.float32), innovation.astype(jnp.float32), precision=lax.Precision.HIGHEST)
    return jnp.concatenate([gram_part, grad_part[None, :]], axis=0)

def patch_quad(states, observed, operator_weight, weights):
    squashed = jnp.tanh(states.astype(jnp.float32)).astype(jnp.bfloat16)
    predicted = jnp.einsum('cr,trm->tcm', operator_weight.astype(jnp.float32), squashed.astype(jnp.float32), precision=lax.Precision.HIGHEST)
    misfit = (predicted - observed[:, :, None]).astype(jnp.bfloat16)
    return quad_terms(misfit, weights)

def inverse_root(gram):
    members = gram.shape[-1]
    identity = jnp.eye(members, dtype=jnp.float32)
    shifted = gram + (members - 1.0) * identity
    norm_size = jnp.sqrt(lax.optimization_barrier(jnp.sum(shifted * shifted, axis=(1, 2))))
    iterate = shifted / norm_size[:, None, None]
    factor = jnp.broadcast_to(identity, gram.shape)
    for number in range(NS_STEPS):
        middle = 1.5 * identity - 0.5 * jnp.einsum('bij,bjk->bik', factor, iterate, precision=lax.Precision.HIGHEST)
        iterate = jnp.einsum('bij,bjk->bik', iterate, middle, precision=lax.Precision.HIGHEST)
        factor = jnp.einsum('bij,bjk->bik', middle, factor, precision=lax.Precision.HIGHEST)
    return factor / jnp.sqrt(norm_size)[:, None, None]

def transform(totals):
    members = totals.shape[-1]
    gram = totals[:, :members, :]
    grad = totals[:, members, :]
    inv_root = inverse_root(gram)
    inner = jnp.einsum('bij,bj->bi', inv_root, grad, precision=lax.Precision.HIGHEST)
    along = jnp.einsum('bij,bj->bi', inv_root, inner, precision=lax.Precision.HIGHEST)
    return (jnp.sqrt(members - 1.0) * inv_root + along[:, :, None]).astype(jnp.bfloat16)

def apply_mixing(states, mixing):
    centre = lax.optimization_barrier(jnp.mean(states.astype(jnp.float32), axis=-1, keepdims=True))
    deviation = (states.astype(jnp.float32) - centre).astype(jnp.bfloat16)
    moved = jnp.einsum('trm,mn->trn', deviation.astype(jnp.float32), mixing.astype(jnp.float32), precision=lax.Precision.HIGHEST)
    return (centre + moved).astype(jnp.bfloat16)

def reference(ensemble, observations, operator_weight, obs_precision, channel_mask):
    weights = obs_precision[None, :] * channel_mask.astype(jnp.float32) / OUTER
    states = jnp.moveaxis(ensemble, 1, 0)
    observed = jnp.moveaxis(observations, 1, 0)
    for outer_step in range(OUTER):
        quads = lax.map(lambda packed: patch_quad(packed[0], packed[1], operator_weight, weights), (states, observed))
        localized = quads + LOCAL_WEIGHT * (jnp.roll(quads, 1, axis=0) + jnp.roll(quads, -1, axis=0))
        mixing = transform(localized)
        states = lax.map(lambda packed: apply_mixing(packed[0], packed[1]), (states, mixing))
    return jnp.moveaxis(states, 0, 1)
```

```python
import functools
import math

import jax
import jax.numpy as jnp
from jax import lax
from jax.experimental import pallas as pl
from jax.experimental.pallas import tpu as pltpu
from jax.sharding import PartitionSpec as P

OUTER = 2
NS_STEPS = 8
NS_SPLIT = 4
LOCAL_WEIGHT = 0.5
F32 = jnp.float32
BF16 = jnp.bfloat16
VMEM_LIMIT = 28 * 1024 * 1024


def dot(a, b):
    return lax.dot_general(a, b, (((1,), (0,)), ((), ())), preferred_element_type=F32)


def dot_nt(a, b):
    return lax.dot_general(a, b, (((1,), (1,)), ((), ())), preferred_element_type=F32)


def split(x):
    hi = x.astype(BF16)
    return hi, (x - hi.astype(F32)).astype(BF16)


def cat(parts, axis):
    return jnp.concatenate(parts, axis=axis)


def iotas(m):
    return (
        lax.broadcasted_iota(jnp.int32, (m, m), 0),
        lax.broadcasted_iota(jnp.int32, (m, m), 1),
    )


def prepare(obs_ref, prec_ref, mask_ref, rw_ref, ow_ref):
    slots, patches, channels = obs_ref.shape
    members = rw_ref.shape[-1]
    pad = ow_ref.shape[0] - patches
    for t in range(slots):
        weight = prec_ref[...] * mask_ref[t : t + 1, :].astype(F32) / OUTER
        root = jnp.sqrt(weight)
        rw_ref[t] = jnp.broadcast_to(root, (members, channels)).T
        rows = (obs_ref[t] * root).astype(F32)
        if pad:
            rows = cat([rows, jnp.zeros((pad, channels), F32)], 0)
        ow_ref[:, t * channels : (t + 1) * channels] = rows.astype(BF16)


def quads(items, squash, w_ref, rw_ref, ow_ref, store, sq_s, x_s):
    slots, channels, members = rw_ref.shape

    def stage_a(i):
        for t in range(slots):
            sq_s[i, :, t * members : (t + 1) * members] = squash(items[i], t)

    def stage_b(i):
        predicted = dot(w_ref[...], sq_s[i])
        for t in range(slots):
            part = predicted[:, t * members : (t + 1) * members]
            x_s[i, t * channels : (t + 1) * channels, :] = (part * rw_ref[t]).astype(BF16)

    def stage_c(i):
        x = x_s[i]
        left = cat([x.T, ow_ref[...]], 0)
        both = dot(left, x)
        square = both[:members]
        tail = both[members:]
        rows = lax.broadcasted_iota(jnp.int32, tail.shape, 0)
        inner = jnp.sum(jnp.where(rows == items[i], tail, 0.0), axis=0, keepdims=True)
        scale = 1.0 / members
        row = jnp.sum(square, axis=0, keepdims=True) * scale
        col = jnp.sum(square, axis=1, keepdims=True) * scale
        total = jnp.sum(row, axis=1, keepdims=True) * scale
        diff = inner - row
        grad = diff - jnp.sum(diff, axis=1, keepdims=True) * scale
        store(items[i], square - row - (col - total), grad)

    n = len(items)
    for i in range(n + 2):
        if i < n:
            stage_a(i)
        if 0 <= i - 1 < n:
            stage_b(i - 1)
        if 0 <= i - 2 < n:
            stage_c(i - 2)


def edge_messages(odd, q_ref, qg_ref, far_ref, near_ref):
    last = q_ref.shape[0] - 1
    members = q_ref.shape[-1]
    pad = jnp.zeros((far_ref.shape[0] - members - 1, members), F32)
    low = cat([q_ref[0], qg_ref[0:1], pad], 0)
    high = cat([q_ref[last], qg_ref[last : last + 1], pad], 0)
    far_ref[...] = jnp.where(odd, high, low).astype(BF16)
    near_ref[...] = jnp.where(odd, low, high).astype(BF16)


def localize(odd, q_ref, qg_ref, far_ref, near_ref):
    patches, members = q_ref.shape[0], q_ref.shape[-1]
    far = far_ref[...].astype(F32)
    near = near_ref[...].astype(F32)
    left = jnp.where(odd, near, far)
    right = jnp.where(odd, far, near)
    grams = [left[:members]] + [q_ref[p] for p in range(patches)] + [right[:members]]
    grads = [left[members : members + 1]] + [qg_ref[p : p + 1] for p in range(patches)] + [right[members : members + 1]]
    mix = lambda v, p: v[p + 1] + LOCAL_WEIGHT * (v[p] + v[p + 2])
    return [mix(grams, p) for p in range(patches)], [mix(grads, p) for p in range(patches)]


def pack(grams, grads, out_ref):
    patches, members = len(grams), grams[0].shape[0]
    rid, cid = iotas(members)
    half = patches // 2
    rows = []
    for k in range(half):
        a, b = grams[k], grams[k + half]
        out_ref[k * members : (k + 1) * members] = jnp.where(rid <= cid, a, b).astype(BF16)
        rows.append(jnp.sum(jnp.where(rid == cid, b, 0.0), axis=0, keepdims=True))
    rows += list(grads)
    extra = out_ref.shape[0] - half * members
    rows.append(jnp.zeros((extra - len(rows), members), F32))
    out_ref[half * members :] = cat(rows, 0).astype(BF16)


def unpack(in_ref, patches):
    members = in_ref.shape[1]
    rid, cid = iotas(members)
    half = patches // 2
    rows = in_ref[half * members :].astype(F32)
    grams = [None] * patches
    for k in range(half):
        x = in_ref[k * members : (k + 1) * members].astype(F32)
        xt = x.T
        diag = rows[k : k + 1]
        grams[k] = jnp.where(rid <= cid, x, xt)
        grams[k + half] = jnp.where(rid > cid, x, jnp.where(rid < cid, xt, diag))
    return grams, [rows[half + p : half + p + 1] for p in range(patches)]


def inverse_roots(grams, grads):
    members = grams[0].shape[0]
    n = len(grams)
    every = range(n)
    rid, cid = iotas(members)
    identity = jnp.where(rid == cid, 1.0, 0.0).astype(F32)
    zero = jnp.zeros((members, members), BF16)
    shifted = [g + (members - 1.0) * identity for g in grams]
    square = [jnp.sum(jnp.sum(s * s, axis=0, keepdims=True), axis=1, keepdims=True) for s in shifted]
    norm = [jnp.sqrt(s) for s in square]
    t = [shifted[i] * (1.0 / norm[i]) for i in every]
    z = [None] * n
    for step in range(NS_SPLIT):
        sp = [split(v) for v in t]
        if step == 0:
            prod = [
                dot(cat([h, l], 1), cat([cat([h, l], 1), cat([h, zero], 1)], 0)) for h, l in sp
            ]
            sq = [v[:, :members] + v[:, members:] for v in prod]
            z = [1.5 * identity - 0.5 * v for v in t]
        else:
            zs = [split(v) for v in z]
            prod = []
            for (h, l), (zh, zl) in zip(sp, zs):
                top = cat([h, zh], 1)
                prod.append(dot(cat([h, l], 1), cat([top, top], 0)) + dot(h, cat([l, zl], 1)))
            sq = [v[:, :members] for v in prod]
            z = [1.5 * z[i] - 0.5 * prod[i][:, members:] for i in every]
        x = [split(1.5 * t[i] - 0.25 * sq[i]) for i in every]
        prod = [
            dot(cat([x[i][0], x[i][1]], 1), cat([cat(sp[i], 1), cat([sp[i][0], zero], 1)], 0))
            for i in every
        ]
        t = [2.25 * t[i] - (prod[i][:, :members] + prod[i][:, members:]) for i in every]
    d = [identity - v for v in t]
    for step in range(NS_SPLIT, NS_STEPS):
        dh = [v.astype(BF16) for v in d]
        if step < NS_STEPS - 1:
            prod = [dot(dh[i], cat([dh[i], z[i].astype(BF16)], 1)) for i in every]
            z = [z[i] + 0.5 * prod[i][:, members:] for i in every]
            d2 = [v[:, :members] for v in prod]
            d = [0.75 * d2[i] + 0.25 * dot(d2[i].astype(BF16), dh[i]) for i in every]
        else:
            z = [z[i] + 0.5 * dot(dh[i], z[i].astype(BF16)) for i in every]

    def rowdot(v, zs):
        h, l = split(jnp.broadcast_to(v, (8, members)))
        both = dot(cat([h, l], 1), cat([cat(zs, 1), cat([zs[0], zero], 1)], 0))
        return (both[:, :members] + both[:, members:])[0:1]

    zs = [split(v) for v in z]
    inner = [rowdot(grads[i], zs[i]) for i in every]
    along = [rowdot(inner[i], zs[i]) / norm[i] for i in every]
    scale = math.sqrt(members - 1.0)
    out = []
    for i in every:
        root = z[i] * (scale / jnp.sqrt(norm[i]))
        col = jnp.sum(root, axis=1, keepdims=True) * (1.0 / members)
        shift = along[i] - jnp.sum(along[i], axis=1, keepdims=True) * (1.0 / members) + 1.0 / members
        out.append((root - col) + shift)
    return out


def first_kernel(odd_ref, states_ref, w_ref, obs_ref, prec_ref, mask_ref,
                 q_ref, qg_ref, far_ref, near_ref, rw_ref, ow_ref, sq_s, x_s):
    prepare(obs_ref, prec_ref, mask_ref, rw_ref, ow_ref)

    def squash(p, t):
        return jnp.tanh(states_ref[t, p].astype(F32)).astype(BF16)

    def store(p, gram, grad):
        q_ref[p] = gram
        qg_ref[p : p + 1] = grad

    quads(list(range(q_ref.shape[0])), squash, w_ref, rw_ref, ow_ref, store, sq_s, x_s)
    edge_messages(odd_ref[0] == 1, q_ref, qg_ref, far_ref, near_ref)


def combine_kernel(odd_ref, q_ref, qg_ref, far_ref, near_ref, loc_ref, locg_ref, msg_ref):
    grams, grads = localize(odd_ref[0] == 1, q_ref, qg_ref, far_ref, near_ref)
    for p in range(len(grams)):
        loc_ref[p] = grams[p]
        locg_ref[p : p + 1] = grads[p]
    pack(grams, grads, msg_ref)


def totals(loc_ref, locg_ref, msg_ref):
    patches = loc_ref.shape[0]
    grams, grads = unpack(msg_ref, patches)
    return (
        [loc_ref[p] + grams[p] for p in range(patches)],
        [locg_ref[p : p + 1] + grads[p] for p in range(patches)],
    )


def moved(states, mixing):
    return dot_nt(states, mixing).astype(BF16)


def middle_kernel(odd_ref, loc_ref, locg_ref, msg_ref, states_ref, w_ref, rw_ref, ow_ref,
                  new_ref, q_ref, qg_ref, far_ref, near_ref, sq_s, x_s):
    mixing = [m.astype(BF16) for m in inverse_roots(*totals(loc_ref, locg_ref, msg_ref))]

    def squash(p, t):
        fresh = moved(states_ref[t, p], mixing[p])
        new_ref[t, p] = fresh
        return jnp.tanh(fresh.astype(F32)).astype(BF16)

    def store(p, gram, grad):
        q_ref[p] = gram
        qg_ref[p : p + 1] = grad

    quads(list(range(q_ref.shape[0])), squash, w_ref, rw_ref, ow_ref, store, sq_s, x_s)
    edge_messages(odd_ref[0] == 1, q_ref, qg_ref, far_ref, near_ref)


def last_kernel(loc_ref, locg_ref, msg_ref, states_ref, out_ref):
    mixing = [m.astype(BF16) for m in inverse_roots(*totals(loc_ref, locg_ref, msg_ref))]
    slots, patches = states_ref.shape[:2]
    for p in range(patches):
        for t in range(slots):
            out_ref[t, p] = moved(states_ref[t, p], mixing[p])


def call(kernel, out_shape, args, scratch=(), smem=True):
    vmem = pl.BlockSpec(memory_space=pltpu.VMEM)
    specs = [vmem] * len(args)
    if smem:
        specs[0] = pl.BlockSpec(memory_space=pltpu.SMEM)
    outs = [jax.ShapeDtypeStruct(s, d) for s, d in out_shape]
    return pl.pallas_call(
        kernel,
        out_shape=outs,
        in_specs=specs,
        out_specs=[vmem] * len(outs),
        scratch_shapes=[pltpu.VMEM(s, d) for s, d in scratch],
        compiler_params=pltpu.CompilerParams(vmem_limit_bytes=VMEM_LIMIT),
    )(*args)


def neighbours(far, near):
    count = lax.axis_size("region")
    mate = [(r, r ^ 1) for r in range(count)]
    cross = [(r, (r + 1) % count if r % 2 else (r - 1) % count) for r in range(count)]
    return lax.ppermute(far, "region", cross), lax.ppermute(near, "region", mate)


def over_slots(msg):
    count = lax.axis_size("slot")
    if count == 2:
        return lax.ppermute(msg, "slot", [(0, 1), (1, 0)])
    mine = msg.astype(F32)
    return (lax.psum(mine, "slot") - mine).astype(BF16)


def shards(ensemble, observations, operator_weight, obs_precision, channel_mask):
    slots, patches, rows, members = ensemble.shape
    channels = operator_weight.shape[0]
    if lax.axis_size("region") % 2 or patches % 2 or patches > 16:
        raise ValueError("unsupported split")
    odd = (lax.axis_index("region") % 2).astype(jnp.int32).reshape(1)
    edge = ((members + 16, members), BF16)
    q = ((patches, members, members), F32)
    qg = ((patches, members), F32)
    extra = -(-(patches // 2 + patches) // 16) * 16
    msg_shape = ((patches // 2 * members + extra, members), BF16)
    scratch = (
        ((patches, rows, slots * members), BF16),
        ((patches, slots * channels, members), BF16),
    )
    rw = ((slots, channels, members), F32)
    ow = ((16, slots * channels), BF16)
    out = (ensemble.shape, BF16)

    gram, grad, far, near, root_w, obs_w = call(
        first_kernel,
        [q, qg, edge, edge, rw, ow],
        (odd, ensemble, operator_weight, observations, obs_precision[None, :], channel_mask),
        scratch,
    )
    states = ensemble
    for step in range(OUTER):
        far, near = neighbours(far, near)
        loc, locg, msg = call(combine_kernel, [q, qg, msg_shape], (odd, gram, grad, far, near))
        msg = over_slots(msg)
        if step < OUTER - 1:
            states, gram, grad, far, near = call(
                middle_kernel,
                [out, q, qg, edge, edge],
                (odd, loc, locg, msg, states, operator_weight, root_w, obs_w),
                scratch,
            )
        else:
            states = call(last_kernel, [out], (loc, locg, msg, states), smem=False)[0]
    return states


def solution(mesh):
    return jax.shard_map(
        shards,
        mesh=mesh,
        in_specs=(
            P("slot", "region", None, None),
            P("slot", "region", None),
            P(),
            P(),
            P("slot", None),
        ),
        out_specs=P("slot", "region", None, None),
        check_vma=False,
    )
```

```python
import functools
import math

import jax
import jax.numpy as jnp
from jax import lax
from jax.experimental import pallas as pl
from jax.experimental.pallas import tpu as pltpu
from jax.sharding import PartitionSpec as P

OUTER = 2
NS_STEPS = 8
NS_SPLIT = 4
LOCAL_WEIGHT = 0.5
F32 = jnp.float32
BF16 = jnp.bfloat16
VMEM_LIMIT = 28 * 1024 * 1024


def dot(a, b):
    return lax.dot_general(a, b, (((1,), (0,)), ((), ())), preferred_element_type=F32)


def dot_nt(a, b):
    return lax.dot_general(a, b, (((1,), (1,)), ((), ())), preferred_element_type=F32)


def split(x):
    hi = x.astype(BF16)
    return hi, (x - hi.astype(F32)).astype(BF16)


def cat(parts, axis):
    return jnp.concatenate(parts, axis=axis)


def iotas(m):
    return (
        lax.broadcasted_iota(jnp.int32, (m, m), 0),
        lax.broadcasted_iota(jnp.int32, (m, m), 1),
    )


def prepare(obs_ref, prec_ref, mask_ref, rw_ref, ow_ref):
    slots, patches, channels = obs_ref.shape
    members = rw_ref.shape[-1]
    pad = ow_ref.shape[0] - patches
    for t in range(slots):
        weight = prec_ref[...] * mask_ref[t : t + 1, :].astype(F32) / OUTER
        root = jnp.sqrt(weight)
        rw_ref[t] = jnp.broadcast_to(root, (members, channels)).T
        rows = (obs_ref[t] * root).astype(F32)
        if pad:
            rows = cat([rows, jnp.zeros((pad, channels), F32)], 0)
        ow_ref[:, t * channels : (t + 1) * channels] = rows.astype(BF16)


def quads(items, squash, w_ref, rw_ref, ow_ref, store, sq_s, x_s):
    slots, channels, members = rw_ref.shape

    def stage_a(i):
        for t in range(slots):
            sq_s[i, :, t * members : (t + 1) * members] = squash(items[i], t)

    def stage_b(i):
        predicted = dot(w_ref[...], sq_s[i])
        for t in range(slots):
            part = predicted[:, t * members : (t + 1) * members]
            x_s[i, t * channels : (t + 1) * channels, :] = (part * rw_ref[t]).astype(BF16)

    def stage_c(i):
        x = x_s[i]
        left = cat([x.T, ow_ref[...]], 0)
        both = dot(left, x)
        square = both[:members]
        tail = both[members:]
        rows = lax.broadcasted_iota(jnp.int32, tail.shape, 0)
        inner = jnp.sum(jnp.where(rows == items[i], tail, 0.0), axis=0, keepdims=True)
        scale = 1.0 / members
        row = jnp.sum(square, axis=0, keepdims=True) * scale
        col = jnp.sum(square, axis=1, keepdims=True) * scale
        total = jnp.sum(row, axis=1, keepdims=True) * scale
        diff = inner - row
        grad = diff - jnp.sum(diff, axis=1, keepdims=True) * scale
        store(items[i], square - row - (col - total), grad)

    n = len(items)
    for i in range(n + 2):
        if i < n:
            stage_a(i)
        if 0 <= i - 1 < n:
            stage_b(i - 1)
        if 0 <= i - 2 < n:
            stage_c(i - 2)


def edges_of(odd, low, high, far_ref, near_ref):
    members = low[0].shape[0]
    pad = jnp.zeros((far_ref.shape[0] - members - 1, members), F32)
    low = cat([low[0], low[1], pad], 0)
    high = cat([high[0], high[1], pad], 0)
    far_ref[...] = jnp.where(odd, high, low).astype(BF16)
    near_ref[...] = jnp.where(odd, low, high).astype(BF16)


def localize(odd, edge_refs, inner_refs, far_ref, near_ref):
    q_edge, qg_edge = edge_refs
    q_inner, qg_inner = inner_refs
    members = q_edge.shape[-1]
    far = far_ref[...].astype(F32)
    near = near_ref[...].astype(F32)
    left = jnp.where(odd, near, far)
    right = jnp.where(odd, far, near)
    inner = q_inner.shape[0]
    grams = [left[:members], q_edge[0]] + [q_inner[p] for p in range(inner)] + [q_edge[1], right[:members]]
    tail = slice(members, members + 1)
    grads = [left[tail], qg_edge[0:1]] + [qg_inner[p : p + 1] for p in range(inner)] + [qg_edge[1:2], right[tail]]
    mix = lambda v, p: v[p + 1] + LOCAL_WEIGHT * (v[p] + v[p + 2])
    return [mix(grams, p) for p in range(inner + 2)], [mix(grads, p) for p in range(inner + 2)]


def pack(grams, grads, out_ref):
    patches, members = len(grams), grams[0].shape[0]
    rid, cid = iotas(members)
    half = patches // 2
    rows = []
    for k in range(half):
        a, b = grams[k], grams[k + half]
        out_ref[k * members : (k + 1) * members] = jnp.where(rid <= cid, a, b).astype(BF16)
        rows.append(jnp.sum(jnp.where(rid == cid, b, 0.0), axis=0, keepdims=True))
    rows += list(grads)
    extra = out_ref.shape[0] - half * members
    rows.append(jnp.zeros((extra - len(rows), members), F32))
    out_ref[half * members :] = cat(rows, 0).astype(BF16)


def unpack(in_ref, patches):
    members = in_ref.shape[1]
    rid, cid = iotas(members)
    half = patches // 2
    rows = in_ref[half * members :].astype(F32)
    grams = [None] * patches
    for k in range(half):
        x = in_ref[k * members : (k + 1) * members].astype(F32)
        xt = x.T
        diag = rows[k : k + 1]
        grams[k] = jnp.where(rid <= cid, x, xt)
        grams[k + half] = jnp.where(rid > cid, x, jnp.where(rid < cid, xt, diag))
    return grams, [rows[half + p : half + p + 1] for p in range(patches)]


def inverse_roots(grams, grads):
    members = grams[0].shape[0]
    n = len(grams)
    every = range(n)
    rid, cid = iotas(members)
    identity = jnp.where(rid == cid, 1.0, 0.0).astype(F32)
    zero = jnp.zeros((members, members), BF16)
    shifted = [g + (members - 1.0) * identity for g in grams]
    square = [jnp.sum(jnp.sum(s * s, axis=0, keepdims=True), axis=1, keepdims=True) for s in shifted]
    norm = [jnp.sqrt(s) for s in square]
    t = [shifted[i] * (1.0 / norm[i]) for i in every]
    z = [None] * n
    for step in range(NS_SPLIT):
        sp = [split(v) for v in t]
        if step == 0:
            prod = [
                dot(cat([h, l], 1), cat([cat([h, l], 1), cat([h, zero], 1)], 0)) for h, l in sp
            ]
            sq = [v[:, :members] + v[:, members:] for v in prod]
            z = [1.5 * identity - 0.5 * v for v in t]
        else:
            zs = [split(v) for v in z]
            prod = []
            for (h, l), (zh, zl) in zip(sp, zs):
                top = cat([h, zh], 1)
                prod.append(dot(cat([h, l], 1), cat([top, top], 0)) + dot(h, cat([l, zl], 1)))
            sq = [v[:, :members] for v in prod]
            z = [1.5 * z[i] - 0.5 * prod[i][:, members:] for i in every]
        x = [split(1.5 * t[i] - 0.25 * sq[i]) for i in every]
        prod = [
            dot(cat([x[i][0], x[i][1]], 1), cat([cat(sp[i], 1), cat([sp[i][0], zero], 1)], 0))
            for i in every
        ]
        t = [2.25 * t[i] - (prod[i][:, :members] + prod[i][:, members:]) for i in every]
    d = [identity - v for v in t]
    for step in range(NS_SPLIT, NS_STEPS):
        dh = [v.astype(BF16) for v in d]
        if step < NS_STEPS - 1:
            prod = [dot(dh[i], cat([dh[i], z[i].astype(BF16)], 1)) for i in every]
            z = [z[i] + 0.5 * prod[i][:, members:] for i in every]
            d2 = [v[:, :members] for v in prod]
            d = [0.75 * d2[i] + 0.25 * dot(d2[i].astype(BF16), dh[i]) for i in every]
        else:
            z = [z[i] + 0.5 * dot(dh[i], z[i].astype(BF16)) for i in every]

    def rowdot(v, zs):
        h, l = split(jnp.broadcast_to(v, (8, members)))
        both = dot(cat([h, l], 1), cat([cat(zs, 1), cat([zs[0], zero], 1)], 0))
        return (both[:, :members] + both[:, members:])[0:1]

    zs = [split(v) for v in z]
    inner = [rowdot(grads[i], zs[i]) for i in every]
    along = [rowdot(inner[i], zs[i]) / norm[i] for i in every]
    scale = math.sqrt(members - 1.0)
    out = []
    for i in every:
        root = z[i] * (scale / jnp.sqrt(norm[i]))
        col = jnp.sum(root, axis=1, keepdims=True) * (1.0 / members)
        shift = along[i] - jnp.sum(along[i], axis=1, keepdims=True) * (1.0 / members) + 1.0 / members
        out.append((root - col) + shift)
    return out


def squash_of(states_ref):
    return lambda p, t: jnp.tanh(states_ref[t, p].astype(F32)).astype(BF16)


def advance(states_ref, mixing_of, new_ref):
    def squash(p, t):
        fresh = dot_nt(states_ref[t, p], mixing_of(p)).astype(BF16)
        new_ref[t, p] = fresh
        return jnp.tanh(fresh.astype(F32)).astype(BF16)

    return squash


def into(q_ref, qg_ref, first):
    def store(p, gram, grad):
        q_ref[p - first] = gram
        qg_ref[p - first : p - first + 1] = grad

    return store


def edge_quads(odd, patches, squash, w_ref, rw_ref, ow_ref, q_ref, qg_ref, far_ref, near_ref, sq_s, x_s):
    ends = [0, patches - 1]
    found = {}

    def store(p, gram, grad):
        found[p] = (gram, grad)
        k = ends.index(p)
        q_ref[k] = gram
        qg_ref[k : k + 1] = grad

    quads(ends, squash, w_ref, rw_ref, ow_ref, store, sq_s, x_s)
    edges_of(odd, found[ends[0]], found[ends[1]], far_ref, near_ref)


def first_kernel(odd_ref, states_hbm, w_hbm, obs_hbm, prec_hbm, mask_hbm,
                 states_ref, w_ref, q_ref, qg_ref, far_ref, near_ref, rw_ref, ow_ref,
                 sq_s, x_s, obs_s, prec_s, mask_s, sems):
    patches = states_ref.shape[1]
    slots = states_ref.shape[0]
    ends = [0, patches - 1]
    small = [
        pltpu.make_async_copy(prec_hbm, prec_s, sems.at[0]),
        pltpu.make_async_copy(mask_hbm, mask_s, sems.at[1]),
        pltpu.make_async_copy(obs_hbm, obs_s, sems.at[2]),
    ]
    weights = pltpu.make_async_copy(w_hbm, w_ref, sems.at[3])
    state = {
        (t, p): pltpu.make_async_copy(
            states_hbm.at[t, p], states_ref.at[t, p], sems.at[4 + t * patches + p]
        )
        for p in range(patches)
        for t in range(slots)
    }
    early = [state[t, p] for p in ends for t in range(slots)]
    for c in early + [weights] + small:
        c.start()
    late = [state[t, p] for p in range(1, patches - 1) for t in range(slots)]
    for c in late:
        c.start()
    for c in early + [weights] + small:
        c.wait()
    prepare(obs_s, prec_s, mask_s, rw_ref, ow_ref)
    edge_quads(odd_ref[0] == 1, patches, squash_of(states_ref), w_ref, rw_ref, ow_ref,
               q_ref, qg_ref, far_ref, near_ref, sq_s, x_s)
    for c in late:
        c.wait()


def inner_kernel(states_ref, w_ref, rw_ref, ow_ref, q_ref, qg_ref, sq_s, x_s):
    items = list(range(1, states_ref.shape[1] - 1))
    quads(items, squash_of(states_ref), w_ref, rw_ref, ow_ref, into(q_ref, qg_ref, 1), sq_s, x_s)


def combine_kernel(odd_ref, qe_ref, qge_ref, qi_ref, qgi_ref, far_ref, near_ref, loc_ref, locg_ref, msg_ref):
    grams, grads = localize(odd_ref[0] == 1, (qe_ref, qge_ref), (qi_ref, qgi_ref), far_ref, near_ref)
    for p in range(len(grams)):
        loc_ref[p] = grams[p]
        locg_ref[p : p + 1] = grads[p]
    pack(grams, grads, msg_ref)


def totals(loc_ref, locg_ref, msg_ref):
    patches = loc_ref.shape[0]
    grams, grads = unpack(msg_ref, patches)
    return (
        [loc_ref[p] + grams[p] for p in range(patches)],
        [locg_ref[p : p + 1] + grads[p] for p in range(patches)],
    )


def root_kernel(odd_ref, loc_ref, locg_ref, msg_ref, states_ref, w_ref, rw_ref, ow_ref,
                mix_ref, new_ref, q_ref, qg_ref, far_ref, near_ref, sq_s, x_s):
    mixing = [m.astype(BF16) for m in inverse_roots(*totals(loc_ref, locg_ref, msg_ref))]
    patches = loc_ref.shape[0]
    for p in range(1, patches - 1):
        mix_ref[p - 1] = mixing[p]
    ends = [0, patches - 1]
    place = lambda ref: _Placed(ref, ends)
    edge_quads(odd_ref[0] == 1, patches, advance(states_ref, lambda p: mixing[p], place(new_ref)),
               w_ref, rw_ref, ow_ref, q_ref, qg_ref, far_ref, near_ref, sq_s, x_s)


class _Placed:
    def __init__(self, ref, items):
        self.ref, self.items = ref, items

    def __setitem__(self, where, value):
        self.ref[where[0], self.items.index(where[1])] = value


def advance_kernel(mix_ref, states_ref, w_ref, rw_ref, ow_ref, new_ref, q_ref, qg_ref, sq_s, x_s):
    items = list(range(1, states_ref.shape[1] - 1))
    squash = advance(states_ref, lambda p: mix_ref[p - 1], _Placed(new_ref, items))
    quads(items, squash, w_ref, rw_ref, ow_ref, into(q_ref, qg_ref, 1), sq_s, x_s)


def last_kernel(loc_ref, locg_ref, msg_ref, *refs):
    *states, out_hbm, out_s, sems = refs
    mixing = [m.astype(BF16) for m in inverse_roots(*totals(loc_ref, locg_ref, msg_ref))]
    slots, patches = out_s.shape[:2]
    copies = []
    for p in range(patches):
        for t in range(slots):
            if len(states) == 1:
                value = states[0][t, p]
            elif p in (0, patches - 1):
                value = states[0][t, min(p, 1)]
            else:
                value = states[1][t, p - 1]
            out_s[t, p] = dot_nt(value, mixing[p]).astype(BF16)
            copies.append(pltpu.make_async_copy(out_s.at[t, p], out_hbm.at[t, p], sems.at[len(copies)]))
            copies[-1].start()
    for c in copies:
        c.wait()


SPACES = {"s": pltpu.SMEM, "v": pltpu.VMEM, "h": pltpu.HBM}


def call(kernel, out_shape, args, kinds, scratch=(), flops=10 ** 9, out_kinds=None):
    outs = [jax.ShapeDtypeStruct(s, d) for s, d in out_shape]
    spec = lambda k: pl.BlockSpec(memory_space=SPACES[k])
    return pl.pallas_call(
        kernel,
        out_shape=outs,
        in_specs=[spec(k) for k in kinds],
        out_specs=[spec(k) for k in (out_kinds or "v" * len(outs))],
        scratch_shapes=[pltpu.VMEM(*s) if isinstance(s, tuple) else s for s in scratch],
        cost_estimate=pl.CostEstimate(flops=flops, bytes_accessed=0, transcendentals=0),
        compiler_params=pltpu.CompilerParams(vmem_limit_bytes=VMEM_LIMIT),
        name=kernel.__name__,
    )(*args)


def neighbours(far, near):
    count = lax.axis_size("region")
    mate = [(r, r ^ 1) for r in range(count)]
    cross = [(r, (r + 1) % count if r % 2 else (r - 1) % count) for r in range(count)]
    return lax.ppermute(far, "region", cross), lax.ppermute(near, "region", mate)


def over_slots(msg):
    count = lax.axis_size("slot")
    if count == 2:
        return lax.ppermute(msg, "slot", [(0, 1), (1, 0)])
    mine = msg.astype(F32)
    return (lax.psum(mine, "slot") - mine).astype(BF16)


def shards(ensemble, observations, operator_weight, obs_precision, channel_mask):
    slots, patches, rows, members = ensemble.shape
    channels = operator_weight.shape[0]
    if lax.axis_size("region") % 2 or patches % 2 or not 4 <= patches <= 16:
        raise ValueError("unsupported split")
    inner = patches - 2
    odd = (lax.axis_index("region") % 2).astype(jnp.int32).reshape(1)
    edge = ((members + 16, members), BF16)
    gram = lambda n: ((n, members, members), F32)
    grad = lambda n: ((n, members), F32)
    extra = -(-(patches // 2 + patches) // 16) * 16
    msg_shape = ((patches // 2 * members + extra, members), BF16)
    scratch = lambda n: (
        ((n, rows, slots * members), BF16),
        ((n, slots * channels, members), BF16),
    )
    rw = ((slots, channels, members), F32)
    ow = ((16, slots * channels), BF16)
    state = lambda n: ((slots, n, rows, members), BF16)
    prec = obs_precision[None, :]
    dma = pltpu.SemaphoreType.DMA
    hbm = lambda x: pltpu.with_memory_space_constraint(x, pltpu.HBM)

    states, weight, qe, qge, far, near, root_w, obs_w = call(
        first_kernel,
        [state(patches), (operator_weight.shape, BF16), gram(2), grad(2), edge, edge, rw, ow],
        (odd, hbm(ensemble), hbm(operator_weight), hbm(observations), hbm(prec), hbm(channel_mask)),
        "shhhhh",
        scratch(2) + (
            (observations.shape, F32),
            (prec.shape, F32),
            (channel_mask.shape, jnp.int32),
            dma((4 + slots * patches,)),
        ),
    )
    far, near = neighbours(far, near)
    qi, qgi = call(
        inner_kernel, [gram(inner), grad(inner)], (states, weight, root_w, obs_w), "vvvv", scratch(inner)
    )
    parts = (states,)
    for step in range(OUTER):
        loc, locg, msg = call(
            combine_kernel,
            [gram(patches), grad(patches), msg_shape],
            (odd, qe, qge, qi, qgi, far, near),
            "svvvvvv",
        )
        msg = over_slots(msg)
        if step == OUTER - 1:
            break
        if len(parts) > 1:
            edges, inside = parts
            states = jnp.concatenate([edges[:, :1], inside, edges[:, 1:]], axis=1)
        mix, edges, qe, qge, far, near = call(
            root_kernel,
            [((inner, members, members), BF16), state(2), gram(2), grad(2), edge, edge],
            (odd, loc, locg, msg, states, weight, root_w, obs_w),
            "svvvvvvv",
            scratch(2),
        )
        far, near = neighbours(far, near)
        inside, qi, qgi = call(
            advance_kernel,
            [state(inner), gram(inner), grad(inner)],
            (mix, states, weight, root_w, obs_w),
            "vvvvv",
            scratch(inner),
        )
        parts = (edges, inside)
    return call(
        last_kernel,
        [state(patches)],
        (loc, locg, msg) + parts,
        "vvv" + "v" * len(parts),
        (state(patches), dma((slots * patches,))),
        out_kinds="h",
    )[0]


def solution(mesh):
    return jax.shard_map(
        shards,
        mesh=mesh,
        in_specs=(
            P("slot", "region", None, None),
            P("slot", "region", None),
            P(),
            P(),
            P("slot", None),
        ),
        out_specs=P("slot", "region", None, None),
        check_vma=False,
    )
```

```python
import functools
import math

import jax
import jax.numpy as jnp
from jax import lax
from jax.experimental import pallas as pl
from jax.experimental.pallas import tpu as pltpu
from jax.sharding import PartitionSpec as P

OUTER = 2
NS_STEPS = 8
NS_SPLIT = 4
LOCAL_WEIGHT = 0.5
F32 = jnp.float32
BF16 = jnp.bfloat16
VMEM_LIMIT = 28 * 1024 * 1024


def dot(a, b):
    return lax.dot_general(a, b, (((1,), (0,)), ((), ())), preferred_element_type=F32)


def dot_nt(a, b):
    return lax.dot_general(a, b, (((1,), (1,)), ((), ())), preferred_element_type=F32)


def split(x):
    hi = x.astype(BF16)
    return hi, (x - hi.astype(F32)).astype(BF16)


def cat(parts, axis):
    return jnp.concatenate(parts, axis=axis)


def iotas(m):
    return (
        lax.broadcasted_iota(jnp.int32, (m, m), 0),
        lax.broadcasted_iota(jnp.int32, (m, m), 1),
    )


def prepare(obs_ref, prec_ref, mask_ref, rw_ref, ow_ref):
    slots, patches, channels = obs_ref.shape
    members = rw_ref.shape[-1]
    pad = ow_ref.shape[0] - patches
    for t in range(slots):
        weight = prec_ref[...] * mask_ref[t : t + 1, :].astype(F32) / OUTER
        root = jnp.sqrt(weight)
        rw_ref[t] = jnp.broadcast_to(root, (members, channels)).T
        rows = (obs_ref[t] * root).astype(F32)
        if pad:
            rows = cat([rows, jnp.zeros((pad, channels), F32)], 0)
        ow_ref[:, t * channels : (t + 1) * channels] = rows.astype(BF16)


def quads(items, squash, w_ref, rw_ref, ow_ref, store, sq_s, x_s, before_a=None, before_b=None):
    slots, channels, members = rw_ref.shape

    def stage_a(i):
        for t in range(slots):
            sq_s[i, :, t * members : (t + 1) * members] = squash(items[i], t)

    def stage_b(i):
        predicted = dot(w_ref[...], sq_s[i])
        for t in range(slots):
            part = predicted[:, t * members : (t + 1) * members]
            x_s[i, t * channels : (t + 1) * channels, :] = (part * rw_ref[t]).astype(BF16)

    def stage_c(i):
        x = x_s[i]
        left = cat([x.T, ow_ref[...]], 0)
        both = dot(left, x)
        square = both[:members]
        tail = both[members:]
        rows = lax.broadcasted_iota(jnp.int32, tail.shape, 0)
        inner = jnp.sum(jnp.where(rows == items[i], tail, 0.0), axis=0, keepdims=True)
        scale = 1.0 / members
        row = jnp.sum(square, axis=0, keepdims=True) * scale
        col = jnp.sum(square, axis=1, keepdims=True) * scale
        total = jnp.sum(row, axis=1, keepdims=True) * scale
        diff = inner - row
        grad = diff - jnp.sum(diff, axis=1, keepdims=True) * scale
        store(items[i], square - row - (col - total), grad)

    n = len(items)
    for i in range(n + 2):
        if i < n:
            if before_a is not None:
                before_a(i)
            stage_a(i)
        if 0 <= i - 1 < n:
            if before_b is not None:
                before_b(i - 1)
            stage_b(i - 1)
        if 0 <= i - 2 < n:
            stage_c(i - 2)


def edges_of(odd, low, high, far_ref, near_ref):
    members = low[0].shape[0]
    pad = jnp.zeros((far_ref.shape[0] - members - 1, members), F32)
    low = cat([low[0], low[1], pad], 0)
    high = cat([high[0], high[1], pad], 0)
    far_ref[...] = jnp.where(odd, high, low).astype(BF16)
    near_ref[...] = jnp.where(odd, low, high).astype(BF16)


def localize(odd, edge_refs, insides, far, near):
    q_edge, qg_edge = edge_refs
    q_inner, qg_inner = insides
    members = q_edge.shape[-1]
    left = jnp.where(odd, near, far)
    right = jnp.where(odd, far, near)
    inner = len(q_inner)
    grams = [left[:members], q_edge[0]] + list(q_inner) + [q_edge[1], right[:members]]
    tail = slice(members, members + 1)
    grads = [left[tail], qg_edge[0:1]] + list(qg_inner) + [qg_edge[1:2], right[tail]]
    mix = lambda v, p: v[p + 1] + LOCAL_WEIGHT * (v[p] + v[p + 2])
    return [mix(grams, p) for p in range(inner + 2)], [mix(grads, p) for p in range(inner + 2)]


def pack(grams, grads, out_ref):
    patches, members = len(grams), grams[0].shape[0]
    rid, cid = iotas(members)
    half = patches // 2
    rows = []
    for k in range(half):
        a, b = grams[k], grams[k + half]
        out_ref[k * members : (k + 1) * members] = jnp.where(rid <= cid, a, b).astype(BF16)
        rows.append(jnp.sum(jnp.where(rid == cid, b, 0.0), axis=0, keepdims=True))
    rows += list(grads)
    extra = out_ref.shape[0] - half * members
    rows.append(jnp.zeros((extra - len(rows), members), F32))
    out_ref[half * members :] = cat(rows, 0).astype(BF16)


def unpack(in_ref, patches):
    members = in_ref.shape[1]
    rid, cid = iotas(members)
    half = patches // 2
    rows = in_ref[half * members :].astype(F32)
    grams = [None] * patches
    for k in range(half):
        x = in_ref[k * members : (k + 1) * members].astype(F32)
        xt = x.T
        diag = rows[k : k + 1]
        grams[k] = jnp.where(rid <= cid, x, xt)
        grams[k + half] = jnp.where(rid > cid, x, jnp.where(rid < cid, xt, diag))
    return grams, [rows[half + p : half + p + 1] for p in range(patches)]


def inverse_roots(grams, grads):
    members = grams[0].shape[0]
    n = len(grams)
    every = range(n)
    rid, cid = iotas(members)
    identity = jnp.where(rid == cid, 1.0, 0.0).astype(F32)
    zero = jnp.zeros((members, members), BF16)
    shifted = [g + (members - 1.0) * identity for g in grams]
    square = [jnp.sum(jnp.sum(s * s, axis=0, keepdims=True), axis=1, keepdims=True) for s in shifted]
    norm = [jnp.sqrt(s) for s in square]
    t = [shifted[i] * (1.0 / norm[i]) for i in every]
    z = [None] * n
    for step in range(NS_SPLIT):
        sp = [split(v) for v in t]
        if step == 0:
            prod = [
                dot(cat([h, l], 1), cat([cat([h, l], 1), cat([h, zero], 1)], 0)) for h, l in sp
            ]
            sq = [v[:, :members] + v[:, members:] for v in prod]
            z = [1.5 * identity - 0.5 * v for v in t]
        else:
            zs = [split(v) for v in z]
            prod = []
            for (h, l), (zh, zl) in zip(sp, zs):
                top = cat([h, zh], 1)
                prod.append(dot(cat([h, l], 1), cat([top, top], 0)) + dot(h, cat([l, zl], 1)))
            sq = [v[:, :members] for v in prod]
            z = [1.5 * z[i] - 0.5 * prod[i][:, members:] for i in every]
        x = [split(1.5 * t[i] - 0.25 * sq[i]) for i in every]
        prod = [
            dot(cat([x[i][0], x[i][1]], 1), cat([cat(sp[i], 1), cat([sp[i][0], zero], 1)], 0))
            for i in every
        ]
        t = [2.25 * t[i] - (prod[i][:, :members] + prod[i][:, members:]) for i in every]
    d = [identity - v for v in t]
    for step in range(NS_SPLIT, NS_STEPS):
        dh = [v.astype(BF16) for v in d]
        if step < NS_STEPS - 1:
            prod = [dot(dh[i], cat([dh[i], z[i].astype(BF16)], 1)) for i in every]
            z = [z[i] + 0.5 * prod[i][:, members:] for i in every]
            d2 = [v[:, :members] for v in prod]
            d = [0.75 * d2[i] + 0.25 * dot(d2[i].astype(BF16), dh[i]) for i in every]
        else:
            z = [z[i] + 0.5 * dot(dh[i], z[i].astype(BF16)) for i in every]

    def rowdot(v, zs):
        h, l = split(jnp.broadcast_to(v, (8, members)))
        both = dot(cat([h, l], 1), cat([cat(zs, 1), cat([zs[0], zero], 1)], 0))
        return (both[:, :members] + both[:, members:])[0:1]

    zs = [split(v) for v in z]
    inner = [rowdot(grads[i], zs[i]) for i in every]
    along = [rowdot(inner[i], zs[i]) / norm[i] for i in every]
    scale = math.sqrt(members - 1.0)
    out = []
    for i in every:
        root = z[i] * (scale / jnp.sqrt(norm[i]))
        col = jnp.sum(root, axis=1, keepdims=True) * (1.0 / members)
        shift = along[i] - jnp.sum(along[i], axis=1, keepdims=True) * (1.0 / members) + 1.0 / members
        out.append((root - col) + shift)
    return out


def squash_of(states_ref):
    return lambda p, t: jnp.tanh(states_ref[t, p].astype(F32)).astype(BF16)


def advance(states_ref, mixing_of, new_ref):
    def squash(p, t):
        fresh = dot_nt(states_ref[t, p], mixing_of(p)).astype(BF16)
        new_ref[t, p] = fresh
        return jnp.tanh(fresh.astype(F32)).astype(BF16)

    return squash


def into(q_ref, qg_ref, first):
    def store(p, gram, grad):
        q_ref[p - first] = gram
        qg_ref[p - first : p - first + 1] = grad

    return store


def edge_quads(odd, patches, squash, w_ref, rw_ref, ow_ref, q_ref, qg_ref, far_ref, near_ref, sq_s, x_s,
               **hooks):
    ends = [0, patches - 1]
    found = {}

    def store(p, gram, grad):
        found[p] = (gram, grad)
        k = ends.index(p)
        q_ref[k] = gram
        qg_ref[k : k + 1] = grad

    quads(ends, squash, w_ref, rw_ref, ow_ref, store, sq_s, x_s, **hooks)
    edges_of(odd, found[ends[0]], found[ends[1]], far_ref, near_ref)


def first_kernel(odd_ref, states_hbm, w_hbm, obs_hbm, prec_hbm, mask_hbm,
                 states_ref, w_ref, q_ref, qg_ref, far_ref, near_ref, rw_ref, ow_ref,
                 sq_s, x_s, obs_s, prec_s, mask_s, sems):
    patches = states_ref.shape[1]
    slots = states_ref.shape[0]
    ends = [0, patches - 1]
    small = [
        pltpu.make_async_copy(prec_hbm, prec_s, sems.at[0]),
        pltpu.make_async_copy(mask_hbm, mask_s, sems.at[1]),
        pltpu.make_async_copy(obs_hbm, obs_s, sems.at[2]),
    ]
    weights = pltpu.make_async_copy(w_hbm, w_ref, sems.at[3])
    state = {
        (t, p): pltpu.make_async_copy(
            states_hbm.at[t, p], states_ref.at[t, p], sems.at[4 + t * patches + p]
        )
        for p in range(patches)
        for t in range(slots)
    }
    for c in small:
        c.start()
    for p in ends:
        for t in range(slots):
            state[t, p].start()
    weights.start()
    late = [state[t, p] for p in range(1, patches - 1) for t in range(slots)]

    def before_a(i):
        for t in range(slots):
            state[t, ends[i]].wait()

    def before_b(i):
        if i == 0:
            for c in small:
                c.wait()
            prepare(obs_s, prec_s, mask_s, rw_ref, ow_ref)
            weights.wait()
            for c in late:
                c.start()

    edge_quads(odd_ref[0] == 1, patches, squash_of(states_ref), w_ref, rw_ref, ow_ref,
               q_ref, qg_ref, far_ref, near_ref, sq_s, x_s, before_a=before_a, before_b=before_b)
    for c in late:
        c.wait()


def inner_kernel(role, odd_ref, far_ref, states_ref, w_ref, rw_ref, ow_ref, q_ref, qg_ref, out_ref, sq_s, x_s):
    items = list(range(1, states_ref.shape[1] - 1))
    out_ref[...] = far_ref[...]

    @pl.when(odd_ref[0] == role)
    def _():
        quads(items, squash_of(states_ref), w_ref, rw_ref, ow_ref, into(q_ref, qg_ref, 1), sq_s, x_s)


def combine_kernel(odd_ref, qe_ref, qge_ref, q0_ref, qg0_ref, q1_ref, qg1_ref, even_ref, odd_in_ref, near_ref,
                   loc_ref, locg_ref, msg_ref):
    odd = odd_ref[0] == 1
    inner = q0_ref.shape[0]
    q = [jnp.where(odd, q1_ref[p], q0_ref[p]) for p in range(inner)]
    qg = [jnp.where(odd, qg1_ref[p : p + 1], qg0_ref[p : p + 1]) for p in range(inner)]
    far = jnp.where(odd, odd_in_ref[...].astype(F32), even_ref[...].astype(F32))
    grams, grads = localize(odd, (qe_ref, qge_ref), (q, qg), far, near_ref[...].astype(F32))
    for p in range(len(grams)):
        loc_ref[p] = grams[p]
        locg_ref[p : p + 1] = grads[p]
    pack(grams, grads, msg_ref)


def totals(loc_ref, locg_ref, msg_ref):
    patches = loc_ref.shape[0]
    grams, grads = unpack(msg_ref, patches)
    return (
        [loc_ref[p] + grams[p] for p in range(patches)],
        [locg_ref[p : p + 1] + grads[p] for p in range(patches)],
    )


def root_kernel(odd_ref, loc_ref, locg_ref, msg_ref, states_ref, w_ref, rw_ref, ow_ref,
                mix_ref, new_ref, q_ref, qg_ref, far_ref, near_ref, sq_s, x_s):
    mixing = [m.astype(BF16) for m in inverse_roots(*totals(loc_ref, locg_ref, msg_ref))]
    patches = loc_ref.shape[0]
    for p in range(1, patches - 1):
        mix_ref[p - 1] = mixing[p]
    ends = [0, patches - 1]
    place = lambda ref: _Placed(ref, ends)
    edge_quads(odd_ref[0] == 1, patches, advance(states_ref, lambda p: mixing[p], place(new_ref)),
               w_ref, rw_ref, ow_ref, q_ref, qg_ref, far_ref, near_ref, sq_s, x_s)


class _Placed:
    def __init__(self, ref, items):
        self.ref, self.items = ref, items

    def __setitem__(self, where, value):
        self.ref[where[0], self.items.index(where[1])] = value


def advance_kernel(role, odd_ref, far_ref, mix_ref, states_ref, w_ref, rw_ref, ow_ref,
                   new_ref, q_ref, qg_ref, out_ref, sq_s, x_s):
    items = list(range(1, states_ref.shape[1] - 1))
    out_ref[...] = far_ref[...]

    @pl.when(odd_ref[0] == role)
    def _():
        squash = advance(states_ref, lambda p: mix_ref[p - 1], _Placed(new_ref, items))
        quads(items, squash, w_ref, rw_ref, ow_ref, into(q_ref, qg_ref, 1), sq_s, x_s)


def last_kernel(odd_ref, loc_ref, locg_ref, msg_ref, edges_ref, even_ref, odd_in_ref, out_hbm, out_s, sems):
    mixing = [m.astype(BF16) for m in inverse_roots(*totals(loc_ref, locg_ref, msg_ref))]
    odd = odd_ref[0] == 1
    slots, patches = out_s.shape[:2]
    copies = []
    for p in range(patches):
        for t in range(slots):
            if p in (0, patches - 1):
                value = edges_ref[t, min(p, 1)]
            else:
                value = jnp.where(odd, odd_in_ref[t, p - 1], even_ref[t, p - 1])
            out_s[t, p] = dot_nt(value, mixing[p]).astype(BF16)
            copies.append(pltpu.make_async_copy(out_s.at[t, p], out_hbm.at[t, p], sems.at[len(copies)]))
            copies[-1].start()
    for c in copies:
        c.wait()


SPACES = {"s": pltpu.SMEM, "v": pltpu.VMEM, "h": pltpu.HBM}


def call(kernel, out_shape, args, kinds, scratch=(), flops=10 ** 9, out_kinds=None):
    outs = [jax.ShapeDtypeStruct(s, d) for s, d in out_shape]
    spec = lambda k: pl.BlockSpec(memory_space=SPACES[k])
    return pl.pallas_call(
        kernel,
        out_shape=outs,
        in_specs=[spec(k) for k in kinds],
        out_specs=[spec(k) for k in (out_kinds or "v" * len(outs))],
        scratch_shapes=[pltpu.VMEM(*s) if isinstance(s, tuple) else s for s in scratch],
        cost_estimate=pl.CostEstimate(flops=flops, bytes_accessed=0, transcendentals=0),
        compiler_params=pltpu.CompilerParams(vmem_limit_bytes=VMEM_LIMIT),
        name=getattr(kernel, "func", kernel).__name__,
    )(*args)


def exchange(far, near, between):
    count = lax.axis_size("region")
    mate = [(r, r ^ 1) for r in range(count)]
    up = [(r, (r + 1) % count) for r in range(1, count, 2)]
    down = [(r, (r - 1) % count) for r in range(0, count, 2)]
    near = lax.ppermute(near, "region", mate)
    even_in = lax.ppermute(far, "region", up)
    *first, far = between(0, far)
    odd_in = lax.ppermute(far, "region", down)
    *second, _ = between(1, far)
    return first, second, (even_in, odd_in, near)


def over_slots(msg):
    count = lax.axis_size("slot")
    if count == 2:
        return lax.ppermute(msg, "slot", [(0, 1), (1, 0)])
    mine = msg.astype(F32)
    return (lax.psum(mine, "slot") - mine).astype(BF16)


def shards(ensemble, observations, operator_weight, obs_precision, channel_mask):
    slots, patches, rows, members = ensemble.shape
    channels = operator_weight.shape[0]
    if lax.axis_size("region") % 2 or patches % 2 or not 4 <= patches <= 16:
        raise ValueError("unsupported split")
    inner = patches - 2
    odd = (lax.axis_index("region") % 2).astype(jnp.int32).reshape(1)
    edge = ((members + 16, members), BF16)
    gram = lambda n: ((n, members, members), F32)
    grad = lambda n: ((n, members), F32)
    extra = -(-(patches // 2 + patches) // 16) * 16
    msg_shape = ((patches // 2 * members + extra, members), BF16)
    scratch = lambda n: (
        ((n, rows, slots * members), BF16),
        ((n, slots * channels, members), BF16),
    )
    rw = ((slots, channels, members), F32)
    ow = ((16, slots * channels), BF16)
    state = lambda n: ((slots, n, rows, members), BF16)
    prec = obs_precision[None, :]
    dma = pltpu.SemaphoreType.DMA
    hbm = lambda x: pltpu.with_memory_space_constraint(x, pltpu.HBM)

    states, weight, qe, qge, far, near, root_w, obs_w = call(
        first_kernel,
        [state(patches), (operator_weight.shape, BF16), gram(2), grad(2), edge, edge, rw, ow],
        (odd, hbm(ensemble), hbm(operator_weight), hbm(observations), hbm(prec), hbm(channel_mask)),
        "shhhhh",
        scratch(2) + (
            (observations.shape, F32),
            (prec.shape, F32),
            (channel_mask.shape, jnp.int32),
            dma((4 + slots * patches,)),
        ),
    )
    def plain(role, far):
        return call(
            functools.partial(inner_kernel, role),
            [gram(inner), grad(inner), edge],
            (odd, far, states, weight, root_w, obs_w),
            "svvvvv",
            scratch(inner),
        )

    first, second, received = exchange(far, near, plain)
    for step in range(OUTER):
        loc, locg, msg = call(
            combine_kernel,
            [gram(patches), grad(patches), msg_shape],
            (odd, qe, qge, *first[-2:], *second[-2:], *received),
            "s" + "v" * 9,
        )
        msg = over_slots(msg)
        if step == OUTER - 1:
            break
        if step:
            inside = jnp.where(odd == 1, second[0], first[0])
            states = jnp.concatenate([edges[:, :1], inside, edges[:, 1:]], axis=1)
        mix, edges, qe, qge, far, near = call(
            root_kernel,
            [((inner, members, members), BF16), state(2), gram(2), grad(2), edge, edge],
            (odd, loc, locg, msg, states, weight, root_w, obs_w),
            "svvvvvvv",
            scratch(2),
        )

        def moving(role, far):
            return call(
                functools.partial(advance_kernel, role),
                [state(inner), gram(inner), grad(inner), edge],
                (odd, far, mix, states, weight, root_w, obs_w),
                "svvvvvv",
                scratch(inner),
            )

        first, second, received = exchange(far, near, moving)
    return call(
        last_kernel,
        [state(patches)],
        (odd, loc, locg, msg, edges, first[0], second[0]),
        "svvvvvv",
        (state(patches), dma((slots * patches,))),
        out_kinds="h",
    )[0]


def solution(mesh):
    return jax.shard_map(
        shards,
        mesh=mesh,
        in_specs=(
            P("slot", "region", None, None),
            P("slot", "region", None),
            P(),
            P(),
            P("slot", None),
        ),
        out_specs=P("slot", "region", None, None),
        check_vma=False,
    )
```

```python
import functools
import math

import jax
import jax.numpy as jnp
from jax import lax
from jax.experimental import pallas as pl
from jax.experimental.pallas import tpu as pltpu
from jax.sharding import PartitionSpec as P

OUTER = 2
NS_STEPS = 8
NS_SPLIT = 4
LOCAL_WEIGHT = 0.5
F32 = jnp.float32
BF16 = jnp.bfloat16
VMEM_LIMIT = 28 * 1024 * 1024


def dot(a, b):
    return lax.dot_general(a, b, (((1,), (0,)), ((), ())), preferred_element_type=F32)


def dot_nt(a, b):
    return lax.dot_general(a, b, (((1,), (1,)), ((), ())), preferred_element_type=F32)


def cat(parts, axis):
    return jnp.concatenate(parts, axis=axis)


def iotas(m):
    return (
        lax.broadcasted_iota(jnp.int32, (m, m), 0),
        lax.broadcasted_iota(jnp.int32, (m, m), 1),
    )


def prepare(obs_ref, prec_ref, mask_ref, rw_ref, ow_ref):
    slots, patches, channels = obs_ref.shape
    members = rw_ref.shape[-1]
    pad = ow_ref.shape[0] - patches
    for t in range(slots):
        weight = prec_ref[...] * mask_ref[t : t + 1, :].astype(F32) / OUTER
        root = jnp.sqrt(weight)
        rw_ref[t] = jnp.broadcast_to(root, (members, channels)).T
        rows = (obs_ref[t] * root).astype(F32)
        if pad:
            rows = cat([rows, jnp.zeros((pad, channels), F32)], 0)
        ow_ref[:, t * channels : (t + 1) * channels] = rows.astype(BF16)


def quads(items, squash, w_ref, rw_ref, ow_ref, store, sq_s, x_s, before_a=None, before_b=None):
    slots, channels, members = rw_ref.shape

    def stage_a(i):
        for t in range(slots):
            sq_s[i, :, t * members : (t + 1) * members] = squash(items[i], t)

    def stage_b(i):
        predicted = dot(w_ref[...], sq_s[i])
        for t in range(slots):
            part = predicted[:, t * members : (t + 1) * members]
            x_s[i, t * channels : (t + 1) * channels, :] = (part * rw_ref[t]).astype(BF16)

    def stage_c(i):
        x = x_s[i]
        left = cat([x.T, ow_ref[...]], 0)
        both = dot(left, x)
        square = both[:members]
        tail = both[members:]
        rows = lax.broadcasted_iota(jnp.int32, tail.shape, 0)
        inner = jnp.sum(jnp.where(rows == items[i], tail, 0.0), axis=0, keepdims=True)
        scale = 1.0 / members
        row = jnp.sum(square, axis=0, keepdims=True) * scale
        col = jnp.sum(square, axis=1, keepdims=True) * scale
        total = jnp.sum(row, axis=1, keepdims=True) * scale
        diff = inner - row
        grad = diff - jnp.sum(diff, axis=1, keepdims=True) * scale
        store(items[i], square - row - (col - total), grad)

    n = len(items)
    for i in range(n + 1):
        if i < n:
            if before_a is not None:
                before_a(i)
            stage_a(i)
        if i:
            if before_b is not None:
                before_b(i - 1)
            stage_b(i - 1)
    for i in range(n):
        stage_c(i)


def edges_of(odd, low, high, far_ref, near_ref):
    members = low[0].shape[0]
    pad = jnp.zeros((far_ref.shape[0] - members - 1, members), F32)
    low = cat([low[0], low[1], pad], 0)
    high = cat([high[0], high[1], pad], 0)
    far_ref[...] = jnp.where(odd, high, low).astype(BF16)
    near_ref[...] = jnp.where(odd, low, high).astype(BF16)


def localize(odd, edge_refs, inner_refs, far_ref, near_ref):
    q_edge, qg_edge = edge_refs
    q_inner, qg_inner = inner_refs
    members = q_edge.shape[-1]
    far = far_ref[...].astype(F32)
    near = near_ref[...].astype(F32)
    left = jnp.where(odd, near, far)
    right = jnp.where(odd, far, near)
    inner = q_inner.shape[0]
    grams = [left[:members], q_edge[0]] + [q_inner[p] for p in range(inner)] + [q_edge[1], right[:members]]
    tail = slice(members, members + 1)
    grads = [left[tail], qg_edge[0:1]] + [qg_inner[p : p + 1] for p in range(inner)] + [qg_edge[1:2], right[tail]]
    mix = lambda v, p: v[p + 1] + LOCAL_WEIGHT * (v[p] + v[p + 2])
    return [mix(grams, p) for p in range(inner + 2)], [mix(grads, p) for p in range(inner + 2)]


def pack(grams, grads, out_ref):
    patches, members = len(grams), grams[0].shape[0]
    rid, cid = iotas(members)
    half = patches // 2
    rows = []
    for k in range(half):
        a, b = grams[k], grams[k + half]
        out_ref[k * members : (k + 1) * members] = jnp.where(rid <= cid, a, b).astype(BF16)
        rows.append(jnp.sum(jnp.where(rid == cid, b, 0.0), axis=0, keepdims=True))
    rows += list(grads)
    extra = out_ref.shape[0] - half * members
    rows.append(jnp.zeros((extra - len(rows), members), F32))
    out_ref[half * members :] = cat(rows, 0).astype(BF16)


def unpack(in_ref, patches):
    members = in_ref.shape[1]
    rid, cid = iotas(members)
    half = patches // 2
    rows = in_ref[half * members :].astype(F32)
    grams = [None] * patches
    for k in range(half):
        x = in_ref[k * members : (k + 1) * members].astype(F32)
        xt = x.T
        diag = rows[k : k + 1]
        grams[k] = jnp.where(rid <= cid, x, xt)
        grams[k + half] = jnp.where(rid > cid, x, jnp.where(rid < cid, xt, diag))
    return grams, [rows[half + p : half + p + 1] for p in range(patches)]


def inverse_roots(grams, grads):
    members = grams[0].shape[0]
    every = range(len(grams))
    rid, cid = iotas(members)
    identity = jnp.where(rid == cid, 1.0, 0.0).astype(F32)
    shifted = [g + (members - 1.0) * identity for g in grams]
    square = [jnp.sum(jnp.sum(s * s, axis=0, keepdims=True), axis=1, keepdims=True) for s in shifted]
    norm = [jnp.sqrt(s) for s in square]
    t = [shifted[i] * (1.0 / norm[i]) for i in every]
    y = [jnp.broadcast_to(g, (8, members)) for g in grads]

    def with_row(mat, row):
        high = row.astype(BF16).astype(F32)
        return cat([mat, cat([high, row - high], 0).astype(BF16)], 0)

    def row_of(prod):
        return prod[members : members + 8, :members] + prod[members + 8 :, :members]

    def in_pairs(left, right):
        out = []
        for i in range(0, len(left), 2):
            zero = jnp.zeros_like(right[i])
            both = cat([cat([right[i], zero], 1), cat([zero, right[i + 1]], 1)], 0)
            prod = dot(cat(left[i : i + 2], 1), both)
            out += [prod[:, :members], prod[:, members:]]
        return out

    z = [None for _ in every]
    for step in range(NS_SPLIT):
        th = [v.astype(BF16) for v in t]
        if step == 0:
            prod = [dot(with_row(th[i], y[i]), th[i]) for i in every]
            z = [1.5 * identity - 0.5 * v for v in t]
        else:
            prod = [dot(with_row(th[i], y[i]), cat([th[i], z[i].astype(BF16)], 1)) for i in every]
            z = [1.5 * z[i] - 0.5 * prod[i][:members, members:] for i in every]
        y = [1.5 * y[i] - 0.5 * row_of(prod[i]) for i in every]
        x = [(1.5 * t[i] - 0.25 * prod[i][:members, :members]).astype(BF16) for i in every]
        shrunk = in_pairs(x, th)
        t = [2.25 * t[i] - shrunk[i] for i in every]
    d = [identity - v for v in t]
    for step in range(NS_SPLIT, NS_STEPS):
        dh = [v.astype(BF16) for v in d]
        prod = [dot(with_row(dh[i], y[i]), cat([dh[i], z[i].astype(BF16)], 1)) for i in every]
        z = [z[i] + 0.5 * prod[i][:members, members:] for i in every]
        y = [y[i] + 0.5 * row_of(prod[i]) for i in every]
        if step < NS_STEPS - 1:
            d2 = [v[:members, :members] for v in prod]
            d3 = in_pairs([v.astype(BF16) for v in d2], dh)
            d = [0.75 * d2[i] + 0.25 * d3[i] for i in every]

    scale = math.sqrt(members - 1.0)
    share = 1.0 / members
    out = []
    for i in every:
        yn = y[i] * (1.0 / norm[i])
        high = yn.astype(BF16).astype(F32)
        rows = dot(cat([high, yn - high], 0).astype(BF16), z[i].astype(BF16))
        along = (rows[:8] + rows[8:])[0:1]
        row = jnp.sum(z[i], axis=0, keepdims=True) * share
        col = jnp.sum(z[i], axis=1, keepdims=True) * share
        level = jnp.sum(yn[0:1] * row, axis=1, keepdims=True)
        out.append((z[i] - col) * (scale / jnp.sqrt(norm[i])) + (along - level + share))
    return out


def squash_of(states_ref):
    return lambda p, t: jnp.tanh(states_ref[t, p].astype(F32)).astype(BF16)


def advance(states_ref, mixing_of, new_ref):
    def squash(p, t):
        fresh = dot_nt(states_ref[t, p], mixing_of(p)).astype(BF16)
        new_ref[t, p] = fresh
        return jnp.tanh(fresh.astype(F32)).astype(BF16)

    return squash


def into(q_ref, qg_ref, first):
    def store(p, gram, grad):
        q_ref[p - first] = gram
        qg_ref[p - first : p - first + 1] = grad

    return store


def edge_quads(odd, patches, squash, w_ref, rw_ref, ow_ref, q_ref, qg_ref, far_ref, near_ref, sq_s, x_s,
               **hooks):
    ends = [0, patches - 1]
    found = {}

    def store(p, gram, grad):
        found[p] = (gram, grad)
        k = ends.index(p)
        q_ref[k] = gram
        qg_ref[k : k + 1] = grad

    quads(ends, squash, w_ref, rw_ref, ow_ref, store, sq_s, x_s, **hooks)
    edges_of(odd, found[ends[0]], found[ends[1]], far_ref, near_ref)


def first_kernel(odd_ref, states_hbm, w_hbm, obs_hbm, prec_hbm, mask_hbm,
                 states_ref, w_ref, q_ref, qg_ref, far_ref, near_ref, rw_ref, ow_ref,
                 sq_s, x_s, obs_s, prec_s, mask_s, sems):
    patches = states_ref.shape[1]
    slots = states_ref.shape[0]
    ends = [0, patches - 1]
    small = [
        pltpu.make_async_copy(prec_hbm, prec_s, sems.at[0]),
        pltpu.make_async_copy(mask_hbm, mask_s, sems.at[1]),
        pltpu.make_async_copy(obs_hbm, obs_s, sems.at[2]),
    ]
    weights = pltpu.make_async_copy(w_hbm, w_ref, sems.at[3])
    state = {
        (t, p): pltpu.make_async_copy(
            states_hbm.at[t, p], states_ref.at[t, p], sems.at[4 + t * patches + p]
        )
        for p in range(patches)
        for t in range(slots)
    }
    for c in small:
        c.start()
    for p in ends:
        for t in range(slots):
            state[t, p].start()
    weights.start()
    late = [state[t, p] for p in range(1, patches - 1) for t in range(slots)]
    for c in late:
        c.start()

    def before_a(i):
        for t in range(slots):
            state[t, ends[i]].wait()

    def before_b(i):
        if i == 0:
            for c in small:
                c.wait()
            prepare(obs_s, prec_s, mask_s, rw_ref, ow_ref)
            weights.wait()

    edge_quads(odd_ref[0] == 1, patches, squash_of(states_ref), w_ref, rw_ref, ow_ref,
               q_ref, qg_ref, far_ref, near_ref, sq_s, x_s, before_a=before_a, before_b=before_b)
    for c in late:
        c.wait()


def inner_kernel(states_ref, w_ref, rw_ref, ow_ref, q_ref, qg_ref, sq_s, x_s):
    items = list(range(1, states_ref.shape[1] - 1))
    quads(items, squash_of(states_ref), w_ref, rw_ref, ow_ref, into(q_ref, qg_ref, 1), sq_s, x_s)


def combine_kernel(odd_ref, qe_ref, qge_ref, qi_ref, qgi_ref, far_ref, near_ref, loc_ref, locg_ref, msg_ref):
    grams, grads = localize(odd_ref[0] == 1, (qe_ref, qge_ref), (qi_ref, qgi_ref), far_ref, near_ref)
    for p in range(len(grams)):
        loc_ref[p] = grams[p]
        locg_ref[p : p + 1] = grads[p]
    pack(grams, grads, msg_ref)


def totals(loc_ref, locg_ref, msg_ref):
    patches = loc_ref.shape[0]
    grams, grads = unpack(msg_ref, patches)
    return (
        [loc_ref[p] + grams[p] for p in range(patches)],
        [locg_ref[p : p + 1] + grads[p] for p in range(patches)],
    )


def root_kernel(odd_ref, loc_ref, locg_ref, msg_ref, states_ref, w_ref, rw_ref, ow_ref,
                mix_ref, new_ref, q_ref, qg_ref, far_ref, near_ref, sq_s, x_s):
    mixing = [m.astype(BF16) for m in inverse_roots(*totals(loc_ref, locg_ref, msg_ref))]
    patches = loc_ref.shape[0]
    for p in range(1, patches - 1):
        mix_ref[p - 1] = mixing[p]
    ends = [0, patches - 1]
    place = lambda ref: _Placed(ref, ends)
    edge_quads(odd_ref[0] == 1, patches, advance(states_ref, lambda p: mixing[p], place(new_ref)),
               w_ref, rw_ref, ow_ref, q_ref, qg_ref, far_ref, near_ref, sq_s, x_s)


class _Placed:
    def __init__(self, ref, items):
        self.ref, self.items = ref, items

    def __setitem__(self, where, value):
        self.ref[where[0], self.items.index(where[1])] = value


def advance_kernel(mix_ref, states_ref, w_ref, rw_ref, ow_ref, new_ref, q_ref, qg_ref, sq_s, x_s):
    items = list(range(1, states_ref.shape[1] - 1))
    squash = advance(states_ref, lambda p: mix_ref[p - 1], _Placed(new_ref, items))
    quads(items, squash, w_ref, rw_ref, ow_ref, into(q_ref, qg_ref, 1), sq_s, x_s)


def last_kernel(loc_ref, locg_ref, msg_ref, *refs):
    *states, out_hbm, out_s, sems = refs
    mixing = [m.astype(BF16) for m in inverse_roots(*totals(loc_ref, locg_ref, msg_ref))]
    slots, patches = out_s.shape[:2]
    copies = []
    for p in range(patches):
        for t in range(slots):
            if len(states) == 1:
                value = states[0][t, p]
            elif p in (0, patches - 1):
                value = states[0][t, min(p, 1)]
            else:
                value = states[1][t, p - 1]
            out_s[t, p] = dot_nt(value, mixing[p]).astype(BF16)
            copies.append(pltpu.make_async_copy(out_s.at[t, p], out_hbm.at[t, p], sems.at[len(copies)]))
            copies[-1].start()
    for c in copies:
        c.wait()


SPACES = {"s": pltpu.SMEM, "v": pltpu.VMEM, "h": pltpu.HBM}


def call(kernel, out_shape, args, kinds, scratch=(), flops=10 ** 9, out_kinds=None):
    outs = [jax.ShapeDtypeStruct(s, d) for s, d in out_shape]
    spec = lambda k: pl.BlockSpec(memory_space=SPACES[k])
    return pl.pallas_call(
        kernel,
        out_shape=outs,
        in_specs=[spec(k) for k in kinds],
        out_specs=[spec(k) for k in (out_kinds or "v" * len(outs))],
        scratch_shapes=[pltpu.VMEM(*s) if isinstance(s, tuple) else s for s in scratch],
        cost_estimate=pl.CostEstimate(flops=flops, bytes_accessed=0, transcendentals=0),
        compiler_params=pltpu.CompilerParams(vmem_limit_bytes=VMEM_LIMIT),
        name=kernel.__name__,
    )(*args)


def neighbours(far, near):
    count = lax.axis_size("region")
    mate = [(r, r ^ 1) for r in range(count)]
    cross = [(r, (r + 1) % count if r % 2 else (r - 1) % count) for r in range(count)]
    return lax.ppermute(far, "region", cross), lax.ppermute(near, "region", mate)


def over_slots(msg):
    count = lax.axis_size("slot")
    if count == 2:
        return lax.ppermute(msg, "slot", [(0, 1), (1, 0)])
    mine = msg.astype(F32)
    return (lax.psum(mine, "slot") - mine).astype(BF16)


def shards(ensemble, observations, operator_weight, obs_precision, channel_mask):
    slots, patches, rows, members = ensemble.shape
    channels = operator_weight.shape[0]
    if lax.axis_size("region") % 2 or patches % 2 or not 4 <= patches <= 16:
        raise ValueError("unsupported split")
    inner = patches - 2
    odd = (lax.axis_index("region") % 2).astype(jnp.int32).reshape(1)
    edge = ((members + 16, members), BF16)
    gram = lambda n: ((n, members, members), F32)
    grad = lambda n: ((n, members), F32)
    extra = -(-(patches // 2 + patches) // 16) * 16
    msg_shape = ((patches // 2 * members + extra, members), BF16)
    scratch = lambda n: (
        ((n, rows, slots * members), BF16),
        ((n, slots * channels, members), BF16),
    )
    rw = ((slots, channels, members), F32)
    ow = ((16, slots * channels), BF16)
    state = lambda n: ((slots, n, rows, members), BF16)
    prec = obs_precision[None, :]
    dma = pltpu.SemaphoreType.DMA
    hbm = lambda x: pltpu.with_memory_space_constraint(x, pltpu.HBM)

    states, weight, qe, qge, far, near, root_w, obs_w = call(
        first_kernel,
        [state(patches), (operator_weight.shape, BF16), gram(2), grad(2), edge, edge, rw, ow],
        (odd, hbm(ensemble), hbm(operator_weight), hbm(observations), hbm(prec), hbm(channel_mask)),
        "shhhhh",
        scratch(2) + (
            (observations.shape, F32),
            (prec.shape, F32),
            (channel_mask.shape, jnp.int32),
            dma((4 + slots * patches,)),
        ),
    )
    far, near = neighbours(far, near)
    qi, qgi = call(
        inner_kernel, [gram(inner), grad(inner)], (states, weight, root_w, obs_w), "vvvv", scratch(inner)
    )
    parts = (states,)
    for step in range(OUTER):
        loc, locg, msg = call(
            combine_kernel,
            [gram(patches), grad(patches), msg_shape],
            (odd, qe, qge, qi, qgi, far, near),
            "svvvvvv",
        )
        msg = over_slots(msg)
        if step == OUTER - 1:
            break
        if len(parts) > 1:
            edges, inside = parts
            states = jnp.concatenate([edges[:, :1], inside, edges[:, 1:]], axis=1)
        mix, edges, qe, qge, far, near = call(
            root_kernel,
            [((inner, members, members), BF16), state(2), gram(2), grad(2), edge, edge],
            (odd, loc, locg, msg, states, weight, root_w, obs_w),
            "svvvvvvv",
            scratch(2),
        )
        far, near = neighbours(far, near)
        inside, qi, qgi = call(
            advance_kernel,
            [state(inner), gram(inner), grad(inner)],
            (mix, states, weight, root_w, obs_w),
            "vvvvv",
            scratch(inner),
        )
        parts = (edges, inside)
    return call(
        last_kernel,
        [state(patches)],
        (loc, locg, msg) + parts,
        "vvv" + "v" * len(parts),
        (state(patches), dma((slots * patches,))),
        out_kinds="h",
    )[0]


def solution(mesh):
    return jax.shard_map(
        shards,
        mesh=mesh,
        in_specs=(
            P("slot", "region", None, None),
            P("slot", "region", None),
            P(),
            P(),
            P("slot", None),
        ),
        out_specs=P("slot", "region", None, None),
        check_vma=False,
    )
```

```python
import functools
import math

import jax
import jax.numpy as jnp
from jax import lax
from jax.experimental import pallas as pl
from jax.experimental.pallas import tpu as pltpu
from jax.sharding import PartitionSpec as P

OUTER = 2
NS_STEPS = 8
NS_SPLIT = 4
LOCAL_WEIGHT = 0.5
F32 = jnp.float32
BF16 = jnp.bfloat16
VMEM_LIMIT = 28 * 1024 * 1024


def dot(a, b):
    return lax.dot_general(a, b, (((1,), (0,)), ((), ())), preferred_element_type=F32)


def dot_nt(a, b):
    return lax.dot_general(a, b, (((1,), (1,)), ((), ())), preferred_element_type=F32)


def cat(parts, axis):
    return jnp.concatenate(parts, axis=axis)


def iotas(m):
    return (
        lax.broadcasted_iota(jnp.int32, (m, m), 0),
        lax.broadcasted_iota(jnp.int32, (m, m), 1),
    )


def prepare(obs_ref, prec_ref, mask_ref, rw_ref, ow_ref):
    slots, patches, channels = obs_ref.shape
    members = rw_ref.shape[-1]
    pad = ow_ref.shape[0] - patches
    for t in range(slots):
        weight = prec_ref[...] * mask_ref[t : t + 1, :].astype(F32) / OUTER
        root = jnp.sqrt(weight)
        rw_ref[t] = jnp.broadcast_to(root, (members, channels)).T
        rows = (obs_ref[t] * root).astype(F32)
        if pad:
            rows = cat([rows, jnp.zeros((pad, channels), F32)], 0)
        ow_ref[:, t * channels : (t + 1) * channels] = rows.astype(BF16)


def quads(items, squash, w_ref, rw_ref, ow_ref, store, sq_s, x_s, before_a=None, before_b=None):
    slots, channels, members = rw_ref.shape

    def stage_a(i):
        for t in range(slots):
            sq_s[i, :, t * members : (t + 1) * members] = squash(items[i], t)

    def stage_b(i):
        predicted = dot(w_ref[...], sq_s[i])
        for t in range(slots):
            part = predicted[:, t * members : (t + 1) * members]
            x_s[i, t * channels : (t + 1) * channels, :] = (part * rw_ref[t]).astype(BF16)

    def stage_c(i):
        x = x_s[i]
        left = cat([x.T, ow_ref[...]], 0)
        both = dot(left, x)
        square = both[:members]
        tail = both[members:]
        rows = lax.broadcasted_iota(jnp.int32, tail.shape, 0)
        inner = jnp.sum(jnp.where(rows == items[i], tail, 0.0), axis=0, keepdims=True)
        scale = 1.0 / members
        row = jnp.sum(square, axis=0, keepdims=True) * scale
        col = jnp.sum(square, axis=1, keepdims=True) * scale
        total = jnp.sum(row, axis=1, keepdims=True) * scale
        diff = inner - row
        grad = diff - jnp.sum(diff, axis=1, keepdims=True) * scale
        store(items[i], square - row - (col - total), grad)

    n = len(items)
    for i in range(n + 1):
        if i < n:
            if before_a is not None:
                before_a(i)
            stage_a(i)
        if i:
            if before_b is not None:
                before_b(i - 1)
            stage_b(i - 1)
    for i in range(n):
        stage_c(i)


def edges_of(odd, low, high, far_ref, near_ref):
    members = low[0].shape[0]
    pad = jnp.zeros((far_ref.shape[0] - members - 1, members), F32)
    low = cat([low[0], low[1], pad], 0)
    high = cat([high[0], high[1], pad], 0)
    far_ref[...] = jnp.where(odd, high, low).astype(BF16)
    near_ref[...] = jnp.where(odd, low, high).astype(BF16)


def mixed(v):
    return [v[p + 1] + LOCAL_WEIGHT * (v[p] + v[p + 2]) for p in range(len(v) - 2)]


def pack(grams, grads, out_ref):
    patches, members = len(grams), grams[0].shape[0]
    rid, cid = iotas(members)
    half = patches // 2
    rows = []
    for k in range(half):
        a, b = grams[k], grams[k + half]
        out_ref[k * members : (k + 1) * members] = jnp.where(rid <= cid, a, b).astype(BF16)
        rows.append(jnp.sum(jnp.where(rid == cid, b, 0.0), axis=0, keepdims=True))
    rows += list(grads)
    extra = out_ref.shape[0] - half * members
    rows.append(jnp.zeros((extra - len(rows), members), F32))
    out_ref[half * members :] = cat(rows, 0).astype(BF16)


def unpack(in_ref, patches):
    members = in_ref.shape[1]
    rid, cid = iotas(members)
    half = patches // 2
    rows = in_ref[half * members :].astype(F32)
    grams = [None] * patches
    for k in range(half):
        x = in_ref[k * members : (k + 1) * members].astype(F32)
        xt = x.T
        diag = rows[k : k + 1]
        grams[k] = jnp.where(rid <= cid, x, xt)
        grams[k + half] = jnp.where(rid > cid, x, jnp.where(rid < cid, xt, diag))
    return grams, [rows[half + p : half + p + 1] for p in range(patches)]


def inverse_roots(grams, grads):
    members = grams[0].shape[0]
    every = range(len(grams))
    rid, cid = iotas(members)
    identity = jnp.where(rid == cid, 1.0, 0.0).astype(F32)
    shifted = [g + (members - 1.0) * identity for g in grams]
    square = [jnp.sum(jnp.sum(s * s, axis=0, keepdims=True), axis=1, keepdims=True) for s in shifted]
    norm = [jnp.sqrt(s) for s in square]
    inv = [1.0 / v for v in norm]
    y = [jnp.broadcast_to(g, (8, members)) for g in grads]

    def with_row(mat, row):
        high = row.astype(BF16).astype(F32)
        return cat([mat, cat([high, row - high], 0).astype(BF16)], 0)

    def row_of(prod):
        return prod[members : members + 8, :members] + prod[members + 8 :, :members]

    def in_pairs(left, right):
        out = []
        for i in range(0, len(left), 2):
            zero = jnp.zeros_like(right[i])
            both = cat([cat([right[i], zero], 1), cat([zero, right[i + 1]], 1)], 0)
            prod = dot(cat(left[i : i + 2], 1), both)
            out += [prod[:, :members], prod[:, members:]]
        return out

    z = [None for _ in every]
    for step in range(NS_SPLIT):
        if step == 0:
            th = [v.astype(BF16) for v in shifted]
            prod = [dot(with_row(th[i], y[i]), th[i]) * inv[i] for i in every]
            t = [shifted[i] * inv[i] for i in every]
            square = [prod[i][:members] * inv[i] for i in every]
            z = [1.5 * identity - 0.5 * v for v in t]
        else:
            th = [v.astype(BF16) for v in t]
            prod = [dot(with_row(th[i], y[i]), cat([th[i], z[i].astype(BF16)], 1)) for i in every]
            square = [v[:members, :members] for v in prod]
            z = [1.5 * z[i] - 0.5 * prod[i][:members, members:] for i in every]
        y = [1.5 * y[i] - 0.5 * row_of(prod[i]) for i in every]
        x = [(1.5 * t[i] - 0.25 * square[i]).astype(BF16) for i in every]
        shrunk = in_pairs(x, th)
        if step == 0:
            shrunk = [shrunk[i] * inv[i] for i in every]
        t = [2.25 * t[i] - shrunk[i] for i in every]
    d = [identity - v for v in t]
    for step in range(NS_SPLIT, NS_STEPS):
        dh = [v.astype(BF16) for v in d]
        prod = [dot(with_row(dh[i], y[i]), cat([dh[i], z[i].astype(BF16)], 1)) for i in every]
        z = [z[i] + 0.5 * prod[i][:members, members:] for i in every]
        y = [y[i] + 0.5 * row_of(prod[i]) for i in every]
        if step < NS_STEPS - 1:
            d2 = [v[:members, :members] for v in prod]
            d3 = in_pairs([v.astype(BF16) for v in d2], dh)
            d = [0.75 * d2[i] + 0.25 * d3[i] for i in every]

    scale = math.sqrt(members - 1.0)
    share = 1.0 / members
    out = []
    for i in every:
        yn = y[i] * (1.0 / norm[i])
        high = yn.astype(BF16).astype(F32)
        rows = dot(cat([high, yn - high], 0).astype(BF16), z[i].astype(BF16))
        along = (rows[:8] + rows[8:])[0:1]
        row = jnp.sum(z[i], axis=0, keepdims=True) * share
        col = jnp.sum(z[i], axis=1, keepdims=True) * share
        level = jnp.sum(yn[0:1] * row, axis=1, keepdims=True)
        out.append((z[i] - col) * (scale / jnp.sqrt(norm[i])) + (along - level + share))
    return out


def squash_of(states_ref):
    return lambda p, t: jnp.tanh(states_ref[t, p].astype(F32)).astype(BF16)


def advance(states_ref, mixing_of, new_ref):
    def squash(p, t):
        fresh = dot_nt(states_ref[t, p], mixing_of(p)).astype(BF16)
        new_ref[t, p] = fresh
        return jnp.tanh(fresh.astype(F32)).astype(BF16)

    return squash


def into(q_ref, qg_ref, first):
    def store(p, gram, grad):
        q_ref[p - first] = gram
        qg_ref[p - first : p - first + 1] = grad

    return store


def edge_quads(odd, patches, squash, w_ref, rw_ref, ow_ref, q_ref, qg_ref, far_ref, near_ref, sq_s, x_s,
               **hooks):
    ends = [0, patches - 1]
    found = {}

    def store(p, gram, grad):
        found[p] = (gram, grad)
        k = ends.index(p)
        q_ref[k] = gram
        qg_ref[k : k + 1] = grad

    quads(ends, squash, w_ref, rw_ref, ow_ref, store, sq_s, x_s, **hooks)
    edges_of(odd, found[ends[0]], found[ends[1]], far_ref, near_ref)


def first_kernel(odd_ref, states_hbm, w_hbm, obs_hbm, prec_hbm, mask_hbm,
                 states_ref, w_ref, q_ref, qg_ref, far_ref, near_ref, rw_ref, ow_ref,
                 sq_s, x_s, obs_s, prec_s, mask_s, sems):
    patches = states_ref.shape[1]
    slots = states_ref.shape[0]
    ends = [0, patches - 1]
    small = [
        pltpu.make_async_copy(prec_hbm, prec_s, sems.at[0]),
        pltpu.make_async_copy(mask_hbm, mask_s, sems.at[1]),
        pltpu.make_async_copy(obs_hbm, obs_s, sems.at[2]),
    ]
    weights = pltpu.make_async_copy(w_hbm, w_ref, sems.at[3])
    state = {
        (t, p): pltpu.make_async_copy(
            states_hbm.at[t, p], states_ref.at[t, p], sems.at[4 + t * patches + p]
        )
        for p in range(patches)
        for t in range(slots)
    }
    for c in small:
        c.start()
    for p in ends:
        for t in range(slots):
            state[t, p].start()
    weights.start()
    late = [state[t, p] for p in range(1, patches - 1) for t in range(slots)]

    def before_a(i):
        for t in range(slots):
            state[t, ends[i]].wait()
        if i == 0:
            for c in late:
                c.start()

    def before_b(i):
        if i == 0:
            for c in small:
                c.wait()
            prepare(obs_s, prec_s, mask_s, rw_ref, ow_ref)
            weights.wait()

    edge_quads(odd_ref[0] == 1, patches, squash_of(states_ref), w_ref, rw_ref, ow_ref,
               q_ref, qg_ref, far_ref, near_ref, sq_s, x_s, before_a=before_a, before_b=before_b)
    for c in late:
        c.wait()


def finish_inner(qe_ref, qge_ref, found, outs):
    loc_ref, locg_ref, msg_ref, q_ref, qg_ref = outs
    inner = len(found)
    grams = mixed([qe_ref[0]] + [found[p][0][...] for p in range(inner)] + [qe_ref[1]])
    grads = mixed([qge_ref[0:1]] + [found[p][1] for p in range(inner)] + [qge_ref[1:2]])
    for p in range(inner):
        loc_ref[p] = grams[p]
        locg_ref[p : p + 1] = grads[p]
    pack(grams, grads, msg_ref)
    for k, p in enumerate((0, inner - 1)):
        q_ref[k] = found[p][0][...]
        qg_ref[k : k + 1] = found[p][1]


def inner_quads(items, squash, w_ref, rw_ref, ow_ref, qe_ref, qge_ref, outs, sq_s, x_s, q_s):
    found = []

    def store(p, gram, grad):
        q_s[len(found)] = gram
        found.append((q_s.at[len(found)], grad))

    quads(items, squash, w_ref, rw_ref, ow_ref, store, sq_s, x_s)
    finish_inner(qe_ref, qge_ref, found, outs)


def inner_kernel(states_ref, w_ref, rw_ref, ow_ref, qe_ref, qge_ref, *refs):
    *outs, sq_s, x_s, q_s = refs
    items = list(range(1, states_ref.shape[1] - 1))
    inner_quads(items, squash_of(states_ref), w_ref, rw_ref, ow_ref, qe_ref, qge_ref, outs, sq_s, x_s, q_s)


def combine_kernel(odd_ref, qe_ref, qge_ref, qi_ref, qgi_ref, far_ref, near_ref, loc_ref, locg_ref, msg_ref):
    odd = odd_ref[0] == 1
    members = qe_ref.shape[-1]
    far = far_ref[...].astype(F32)
    near = near_ref[...].astype(F32)
    left = jnp.where(odd, near, far)
    right = jnp.where(odd, far, near)
    tail = slice(members, members + 1)
    grams = mixed([left[:members], qe_ref[0], qi_ref[0]]) + mixed([qi_ref[1], qe_ref[1], right[:members]])
    grads = mixed([left[tail], qge_ref[0:1], qgi_ref[0:1]]) + mixed([qgi_ref[1:2], qge_ref[1:2], right[tail]])
    for k in range(2):
        loc_ref[k] = grams[k]
        locg_ref[k : k + 1] = grads[k]
    pack(grams, grads, msg_ref)


def totals(refs):
    parts = []
    for loc_ref, locg_ref, msg_ref in (refs[:3], refs[3:]):
        n = loc_ref.shape[0]
        grams, grads = unpack(msg_ref, n)
        parts.append(([loc_ref[p] + grams[p] for p in range(n)], [locg_ref[p : p + 1] + grads[p] for p in range(n)]))
    (gi, vi), (ge, ve) = parts
    return ge[:1] + gi + ge[1:], ve[:1] + vi + ve[1:]


def root_kernel(odd_ref, *refs):
    sums, (states_ref, w_ref, rw_ref, ow_ref, mix_ref, new_ref, q_ref, qg_ref, far_ref, near_ref, sq_s, x_s) = (
        refs[:6],
        refs[6:],
    )
    mixing = [m.astype(BF16) for m in inverse_roots(*totals(sums))]
    patches = states_ref.shape[1]
    for p in range(1, patches - 1):
        mix_ref[p - 1] = mixing[p]
    ends = [0, patches - 1]
    place = lambda ref: _Placed(ref, ends)
    edge_quads(odd_ref[0] == 1, patches, advance(states_ref, lambda p: mixing[p], place(new_ref)),
               w_ref, rw_ref, ow_ref, q_ref, qg_ref, far_ref, near_ref, sq_s, x_s)


class _Placed:
    def __init__(self, ref, items):
        self.ref, self.items = ref, items

    def __setitem__(self, where, value):
        self.ref[where[0], self.items.index(where[1])] = value


def advance_kernel(mix_ref, states_ref, w_ref, rw_ref, ow_ref, qe_ref, qge_ref, new_ref, *refs):
    *outs, sq_s, x_s, q_s = refs
    items = list(range(1, states_ref.shape[1] - 1))
    squash = advance(states_ref, lambda p: mix_ref[p - 1], _Placed(new_ref, items))
    inner_quads(items, squash, w_ref, rw_ref, ow_ref, qe_ref, qge_ref, outs, sq_s, x_s, q_s)


def last_kernel(*refs):
    *states, out_hbm, out_s, sems = refs[6:]
    mixing = [m.astype(BF16) for m in inverse_roots(*totals(refs[:6]))]
    slots, patches = out_s.shape[:2]
    copies = []
    for p in range(patches):
        for t in range(slots):
            if len(states) == 1:
                value = states[0][t, p]
            elif p in (0, patches - 1):
                value = states[0][t, min(p, 1)]
            else:
                value = states[1][t, p - 1]
            out_s[t, p] = dot_nt(value, mixing[p]).astype(BF16)
            copies.append(pltpu.make_async_copy(out_s.at[t, p], out_hbm.at[t, p], sems.at[len(copies)]))
            copies[-1].start()
    for c in copies:
        c.wait()


SPACES = {"s": pltpu.SMEM, "v": pltpu.VMEM, "h": pltpu.HBM}


def call(kernel, out_shape, args, kinds, scratch=(), flops=10 ** 9, out_kinds=None):
    outs = [jax.ShapeDtypeStruct(s, d) for s, d in out_shape]
    spec = lambda k: pl.BlockSpec(memory_space=SPACES[k])
    return pl.pallas_call(
        kernel,
        out_shape=outs,
        in_specs=[spec(k) for k in kinds],
        out_specs=[spec(k) for k in (out_kinds or "v" * len(outs))],
        scratch_shapes=[pltpu.VMEM(*s) if isinstance(s, tuple) else s for s in scratch],
        cost_estimate=pl.CostEstimate(flops=flops, bytes_accessed=0, transcendentals=0),
        compiler_params=pltpu.CompilerParams(vmem_limit_bytes=VMEM_LIMIT),
        name=kernel.__name__,
    )(*args)


def neighbours(far, near):
    count = lax.axis_size("region")
    mate = [(r, r ^ 1) for r in range(count)]
    cross = [(r, (r + 1) % count if r % 2 else (r - 1) % count) for r in range(count)]
    return lax.ppermute(far, "region", cross), lax.ppermute(near, "region", mate)


def over_slots(msg):
    count = lax.axis_size("slot")
    if count == 2:
        return lax.ppermute(msg, "slot", [(0, 1), (1, 0)])
    mine = msg.astype(F32)
    return (lax.psum(mine, "slot") - mine).astype(BF16)


def shards(ensemble, observations, operator_weight, obs_precision, channel_mask):
    slots, patches, rows, members = ensemble.shape
    channels = operator_weight.shape[0]
    if lax.axis_size("region") % 2 or patches % 2 or not 4 <= patches <= 16:
        raise ValueError("unsupported split")
    inner = patches - 2
    odd = (lax.axis_index("region") % 2).astype(jnp.int32).reshape(1)
    edge = ((members + 16, members), BF16)
    gram = lambda n: ((n, members, members), F32)
    grad = lambda n: ((n, members), F32)
    message = lambda n: ((n // 2 * members + -(-(n // 2 + n) // 16) * 16, members), BF16)
    inner_out = [gram(inner), grad(inner), message(inner), gram(2), grad(2)]
    inner_scratch = (
        ((inner, rows, slots * members), BF16),
        ((inner, slots * channels, members), BF16),
        gram(inner),
    )
    scratch = lambda n: (
        ((n, rows, slots * members), BF16),
        ((n, slots * channels, members), BF16),
    )
    rw = ((slots, channels, members), F32)
    ow = ((16, slots * channels), BF16)
    state = lambda n: ((slots, n, rows, members), BF16)
    prec = obs_precision[None, :]
    dma = pltpu.SemaphoreType.DMA
    hbm = lambda x: pltpu.with_memory_space_constraint(x, pltpu.HBM)

    states, weight, qe, qge, far, near, root_w, obs_w = call(
        first_kernel,
        [state(patches), (operator_weight.shape, BF16), gram(2), grad(2), edge, edge, rw, ow],
        (odd, hbm(ensemble), hbm(operator_weight), hbm(observations), hbm(prec), hbm(channel_mask)),
        "shhhhh",
        scratch(2) + (
            (observations.shape, F32),
            (prec.shape, F32),
            (channel_mask.shape, jnp.int32),
            dma((4 + slots * patches,)),
        ),
    )
    far, near = neighbours(far, near)
    *loc, msg, qi, qgi = call(
        inner_kernel, inner_out, (states, weight, root_w, obs_w, qe, qge), "vvvvvv", inner_scratch
    )
    parts = (states,)
    for step in range(OUTER):
        sums = (*loc, over_slots(msg))
        *loc, msg = call(
            combine_kernel,
            [gram(2), grad(2), message(2)],
            (odd, qe, qge, qi, qgi, far, near),
            "svvvvvv",
        )
        sums += (*loc, over_slots(msg))
        if step == OUTER - 1:
            break
        if len(parts) > 1:
            edges, inside = parts
            states = jnp.concatenate([edges[:, :1], inside, edges[:, 1:]], axis=1)
        mix, edges, qe, qge, far, near = call(
            root_kernel,
            [((inner, members, members), BF16), state(2), gram(2), grad(2), edge, edge],
            (odd, *sums, states, weight, root_w, obs_w),
            "s" + "v" * 10,
            scratch(2),
        )
        far, near = neighbours(far, near)
        inside, *loc, msg, qi, qgi = call(
            advance_kernel,
            [state(inner)] + inner_out,
            (mix, states, weight, root_w, obs_w, qe, qge),
            "vvvvvvv",
            inner_scratch,
        )
        parts = (edges, inside)
    return call(
        last_kernel,
        [state(patches)],
        sums + parts,
        "v" * (6 + len(parts)),
        (state(patches), dma((slots * patches,))),
        out_kinds="h",
    )[0]


def solution(mesh):
    return jax.shard_map(
        shards,
        mesh=mesh,
        in_specs=(
            P("slot", "region", None, None),
            P("slot", "region", None),
            P(),
            P(),
            P("slot", None),
        ),
        out_specs=P("slot", "region", None, None),
        check_vma=False,
    )
```

```python
import functools
import math

import jax
import jax.numpy as jnp
from jax import lax
from jax.experimental import pallas as pl
from jax.experimental.pallas import tpu as pltpu
from jax.sharding import PartitionSpec as P

OUTER = 2
NS_STEPS = 8
NS_SPLIT = 4
LOCAL_WEIGHT = 0.5
F32 = jnp.float32
BF16 = jnp.bfloat16
VMEM_LIMIT = 28 * 1024 * 1024


def dot(a, b):
    return lax.dot_general(a, b, (((1,), (0,)), ((), ())), preferred_element_type=F32)


def dot_nt(a, b):
    return lax.dot_general(a, b, (((1,), (1,)), ((), ())), preferred_element_type=F32)


def cat(parts, axis):
    return jnp.concatenate(parts, axis=axis)


def iotas(m):
    return (
        lax.broadcasted_iota(jnp.int32, (m, m), 0),
        lax.broadcasted_iota(jnp.int32, (m, m), 1),
    )


def prepare(obs_ref, prec_ref, mask_ref, rw_ref, ow_ref):
    slots, patches, channels = obs_ref.shape
    members = rw_ref.shape[-1]
    pad = ow_ref.shape[0] - patches
    for t in range(slots):
        weight = prec_ref[...] * mask_ref[t : t + 1, :].astype(F32) / OUTER
        root = jnp.sqrt(weight)
        rw_ref[t] = jnp.broadcast_to(root, (members, channels)).T
        rows = (obs_ref[t] * root).astype(F32)
        if pad:
            rows = cat([rows, jnp.zeros((pad, channels), F32)], 0)
        ow_ref[:, t * channels : (t + 1) * channels] = rows.astype(BF16)


def quads(items, squash, w_ref, rw_ref, ow_ref, store, sq_s, xs, before_a=None, before_b=None):
    slots, channels, members = rw_ref.shape
    x_s, xt_s = xs

    def stage_a(i):
        for t in range(slots):
            sq_s[i, :, t * members : (t + 1) * members] = squash(items[i], t)

    def stage_b(i):
        predicted = dot(w_ref[...], sq_s[i])
        for t in range(slots):
            part = predicted[:, t * members : (t + 1) * members]
            x = (part * rw_ref[t]).astype(BF16)
            x_s[i, t * channels : (t + 1) * channels, :] = x
            xt_s[i, :, t * channels : (t + 1) * channels] = x.T

    def stage_c(i):
        x = x_s[i]
        left = cat([xt_s[i], ow_ref[...]], 0)
        both = dot(left, x)
        square = both[:members]
        tail = both[members:]
        rows = lax.broadcasted_iota(jnp.int32, tail.shape, 0)
        inner = jnp.sum(jnp.where(rows == items[i], tail, 0.0), axis=0, keepdims=True)
        scale = 1.0 / members
        row = jnp.sum(square, axis=0, keepdims=True) * scale
        col = jnp.sum(square, axis=1, keepdims=True) * scale
        total = jnp.sum(row, axis=1, keepdims=True) * scale
        diff = inner - row
        grad = diff - jnp.sum(diff, axis=1, keepdims=True) * scale
        store(items[i], square - row - (col - total), grad)

    n = len(items)
    for i in range(n):
        if before_a is not None:
            before_a(i)
        stage_a(i)
    for i in range(n):
        if before_b is not None:
            before_b(i)
        stage_b(i)
    for i in range(n):
        stage_c(i)


def edges_of(odd, low, high, far_ref, near_ref):
    members = low[0].shape[0]
    pad = jnp.zeros((far_ref.shape[0] - members - 1, members), F32)
    low = cat([low[0], low[1], pad], 0)
    high = cat([high[0], high[1], pad], 0)
    far_ref[...] = jnp.where(odd, high, low).astype(BF16)
    near_ref[...] = jnp.where(odd, low, high).astype(BF16)


def mixed(v):
    return [v[p + 1] + LOCAL_WEIGHT * (v[p] + v[p + 2]) for p in range(len(v) - 2)]


def pack(grams, grads, out_ref):
    patches, members = len(grams), grams[0].shape[0]
    rid, cid = iotas(members)
    half = patches // 2
    rows = []
    for k in range(half):
        a, b = grams[k], grams[k + half]
        out_ref[k * members : (k + 1) * members] = jnp.where(rid <= cid, a, b).astype(BF16)
        rows.append(jnp.sum(jnp.where(rid == cid, b, 0.0), axis=0, keepdims=True))
    rows += list(grads)
    extra = out_ref.shape[0] - half * members
    rows.append(jnp.zeros((extra - len(rows), members), F32))
    out_ref[half * members :] = cat(rows, 0).astype(BF16)


def unpack(in_ref, patches):
    members = in_ref.shape[1]
    rid, cid = iotas(members)
    half = patches // 2
    rows = in_ref[half * members :].astype(F32)
    grams = [None] * patches
    for k in range(half):
        x = in_ref[k * members : (k + 1) * members].astype(F32)
        xt = x.T
        diag = rows[k : k + 1]
        grams[k] = jnp.where(rid <= cid, x, xt)
        grams[k + half] = jnp.where(rid > cid, x, jnp.where(rid < cid, xt, diag))
    return grams, [rows[half + p : half + p + 1] for p in range(patches)]


def inverse_roots(shifted, norm, grads):
    members = shifted[0].shape[0]
    every = range(len(shifted))
    rid, cid = iotas(members)
    identity = jnp.where(rid == cid, 1.0, 0.0).astype(F32)
    inv = [1.0 / v for v in norm]
    y = [jnp.broadcast_to(g, (8, members)) for g in grads]

    def with_row(mat, row):
        high = row.astype(BF16).astype(F32)
        return cat([mat, cat([high, row - high], 0).astype(BF16)], 0)

    def row_of(prod):
        return prod[members : members + 8, :members] + prod[members + 8 :, :members]

    def in_pairs(left, right):
        out = []
        for i in range(0, len(left), 2):
            zero = jnp.zeros_like(right[i])
            both = cat([cat([right[i], zero], 1), cat([zero, right[i + 1]], 1)], 0)
            prod = dot(cat(left[i : i + 2], 1), both)
            out += [prod[:, :members], prod[:, members:]]
        return out

    z = [None for _ in every]
    for step in range(NS_SPLIT):
        if step == 0:
            th = [v.astype(BF16) for v in shifted]
            prod = [dot(with_row(th[i], y[i]), th[i]) * inv[i] for i in every]
            t = [shifted[i] * inv[i] for i in every]
            square = [prod[i][:members] * inv[i] for i in every]
            z = [1.5 * identity - 0.5 * v for v in t]
        else:
            th = [v.astype(BF16) for v in t]
            prod = [dot(with_row(th[i], y[i]), cat([th[i], z[i].astype(BF16)], 1)) for i in every]
            square = [v[:members, :members] for v in prod]
            z = [1.5 * z[i] - 0.5 * prod[i][:members, members:] for i in every]
        y = [1.5 * y[i] - 0.5 * row_of(prod[i]) for i in every]
        x = [(1.5 * t[i] - 0.25 * square[i]).astype(BF16) for i in every]
        shrunk = in_pairs(x, th)
        if step == 0:
            shrunk = [shrunk[i] * inv[i] for i in every]
        t = [2.25 * t[i] - shrunk[i] for i in every]
    d = [identity - v for v in t]
    for step in range(NS_SPLIT, NS_STEPS):
        dh = [v.astype(BF16) for v in d]
        prod = [dot(with_row(dh[i], y[i]), cat([dh[i], z[i].astype(BF16)], 1)) for i in every]
        z = [z[i] + 0.5 * prod[i][:members, members:] for i in every]
        y = [y[i] + 0.5 * row_of(prod[i]) for i in every]
        if step < NS_STEPS - 1:
            d2 = [v[:members, :members] for v in prod]
            d3 = in_pairs([v.astype(BF16) for v in d2], dh)
            d = [0.75 * d2[i] + 0.25 * d3[i] for i in every]

    scale = math.sqrt(members - 1.0)
    share = 1.0 / members
    out = []
    for i in every:
        yn = y[i] * (1.0 / norm[i])
        high = yn.astype(BF16).astype(F32)
        rows = dot(cat([high, yn - high], 0).astype(BF16), z[i].astype(BF16))
        along = (rows[:8] + rows[8:])[0:1]
        row = jnp.sum(z[i], axis=0, keepdims=True) * share
        col = jnp.sum(z[i], axis=1, keepdims=True) * share
        level = jnp.sum(yn[0:1] * row, axis=1, keepdims=True)
        out.append((z[i] - col) * (scale / jnp.sqrt(norm[i])) + (along - level + share))
    return out


def squash_of(states_ref):
    return lambda p, t: jnp.tanh(states_ref[t, p].astype(F32)).astype(BF16)


def advance(states_ref, mixing_of, new_ref):
    def squash(p, t):
        fresh = dot_nt(states_ref[t, p], mixing_of(p)).astype(BF16)
        new_ref[t, p] = fresh
        return jnp.tanh(fresh.astype(F32)).astype(BF16)

    return squash


def into(q_ref, qg_ref, first):
    def store(p, gram, grad):
        q_ref[p - first] = gram
        qg_ref[p - first : p - first + 1] = grad

    return store


def edge_quads(odd, patches, squash, w_ref, rw_ref, ow_ref, q_ref, qg_ref, far_ref, near_ref, sq_s, x_s,
               **hooks):
    ends = [0, patches - 1]
    found = {}

    def store(p, gram, grad):
        found[p] = (gram, grad)
        k = ends.index(p)
        q_ref[k] = gram
        qg_ref[k : k + 1] = grad

    quads(ends, squash, w_ref, rw_ref, ow_ref, store, sq_s, x_s, **hooks)
    edges_of(odd, found[ends[0]], found[ends[1]], far_ref, near_ref)


def first_kernel(odd_ref, states_hbm, w_hbm, obs_hbm, prec_hbm, mask_hbm,
                 states_ref, w_ref, q_ref, qg_ref, far_ref, near_ref, rw_ref, ow_ref,
                 sq_s, x_s, obs_s, prec_s, mask_s, sems):
    patches = states_ref.shape[1]
    slots = states_ref.shape[0]
    ends = [0, patches - 1]
    small = [
        pltpu.make_async_copy(prec_hbm, prec_s, sems.at[0]),
        pltpu.make_async_copy(mask_hbm, mask_s, sems.at[1]),
        pltpu.make_async_copy(obs_hbm, obs_s, sems.at[2]),
    ]
    weights = pltpu.make_async_copy(w_hbm, w_ref, sems.at[3])
    state = {
        (t, p): pltpu.make_async_copy(
            states_hbm.at[t, p], states_ref.at[t, p], sems.at[4 + t * patches + p]
        )
        for p in range(patches)
        for t in range(slots)
    }
    for c in small:
        c.start()
    for p in ends:
        for t in range(slots):
            state[t, p].start()
    weights.start()
    late = [state[t, p] for p in range(1, patches - 1) for t in range(slots)]

    def before_a(i):
        for t in range(slots):
            state[t, ends[i]].wait()
        if i == 0:
            for c in late:
                c.start()

    def before_b(i):
        if i == 0:
            for c in small:
                c.wait()
            prepare(obs_s, prec_s, mask_s, rw_ref, ow_ref)
            weights.wait()

    edge_quads(odd_ref[0] == 1, patches, squash_of(states_ref), w_ref, rw_ref, ow_ref,
               q_ref, qg_ref, far_ref, near_ref, sq_s, x_s, before_a=before_a, before_b=before_b)
    for c in late:
        c.wait()


def finish_inner(qe_ref, qge_ref, found, outs):
    loc_ref, locg_ref, msg_ref, q_ref, qg_ref = outs
    inner = len(found)
    grams = mixed([qe_ref[0]] + [found[p][0][...] for p in range(inner)] + [qe_ref[1]])
    grads = mixed([qge_ref[0:1]] + [found[p][1] for p in range(inner)] + [qge_ref[1:2]])
    for p in range(inner):
        loc_ref[p] = grams[p]
        locg_ref[p : p + 1] = grads[p]
    pack(grams, grads, msg_ref)
    for k, p in enumerate((0, inner - 1)):
        q_ref[k] = found[p][0][...]
        qg_ref[k : k + 1] = found[p][1]


def inner_quads(items, squash, w_ref, rw_ref, ow_ref, qe_ref, qge_ref, outs, sq_s, x_s, q_s):
    found = []

    def store(p, gram, grad):
        q_s[len(found)] = gram
        found.append((q_s.at[len(found)], grad))

    quads(items, squash, w_ref, rw_ref, ow_ref, store, sq_s, x_s)
    finish_inner(qe_ref, qge_ref, found, outs)


def inner_kernel(states_ref, w_ref, rw_ref, ow_ref, qe_ref, qge_ref, *refs):
    *outs, sq_s, x_s, q_s = refs
    items = list(range(1, states_ref.shape[1] - 1))
    inner_quads(items, squash_of(states_ref), w_ref, rw_ref, ow_ref, qe_ref, qge_ref, outs, sq_s, x_s, q_s)


def combine_kernel(odd_ref, qe_ref, qge_ref, qi_ref, qgi_ref, far_ref, near_ref, loc_ref, locg_ref, msg_ref):
    odd = odd_ref[0] == 1
    members = qe_ref.shape[-1]
    far = far_ref[...].astype(F32)
    near = near_ref[...].astype(F32)
    left = jnp.where(odd, near, far)
    right = jnp.where(odd, far, near)
    tail = slice(members, members + 1)
    grams = mixed([left[:members], qe_ref[0], qi_ref[0]]) + mixed([qi_ref[1], qe_ref[1], right[:members]])
    grads = mixed([left[tail], qge_ref[0:1], qgi_ref[0:1]]) + mixed([qgi_ref[1:2], qge_ref[1:2], right[tail]])
    for k in range(2):
        loc_ref[k] = grams[k]
        locg_ref[k : k + 1] = grads[k]
    pack(grams, grads, msg_ref)


def shifted_sums(loc_ref, locg_ref, msg_ref):
    n, members = loc_ref.shape[:2]
    rid, cid = iotas(members)
    shift = jnp.where(rid == cid, members - 1.0, 0.0).astype(F32)
    grams, grads = unpack(msg_ref, n)
    shifted = [loc_ref[p] + grams[p] + shift for p in range(n)]
    square = [jnp.sum(jnp.sum(s * s, axis=0, keepdims=True), axis=1, keepdims=True) for s in shifted]
    return shifted, [jnp.sqrt(s) for s in square], [locg_ref[p : p + 1] + grads[p] for p in range(n)]


def sums_kernel(loc_ref, locg_ref, msg_ref, shifted_ref, norm_ref, grad_ref):
    shifted, norm, grads = shifted_sums(loc_ref, locg_ref, msg_ref)
    for p in range(len(grads)):
        shifted_ref[p] = shifted[p]
        norm_ref[p : p + 1] = jnp.broadcast_to(norm[p], grads[p].shape)
        grad_ref[p : p + 1] = grads[p]


def totals(refs):
    shifted_ref, norm_ref, grad_ref = refs[:3]
    shifted, norm, grads = shifted_sums(*refs[3:])
    n = shifted_ref.shape[0]
    return (
        shifted[:1] + [shifted_ref[p] for p in range(n)] + shifted[1:],
        norm[:1] + [norm_ref[p : p + 1, 0:1] for p in range(n)] + norm[1:],
        grads[:1] + [grad_ref[p : p + 1] for p in range(n)] + grads[1:],
    )


def root_kernel(odd_ref, *refs):
    sums, (states_ref, w_ref, rw_ref, ow_ref, mix_ref, new_ref, q_ref, qg_ref, far_ref, near_ref, sq_s, x_s) = (
        refs[:6],
        refs[6:],
    )
    mixing = [m.astype(BF16) for m in inverse_roots(*totals(sums))]
    patches = states_ref.shape[1]
    for p in range(1, patches - 1):
        mix_ref[p - 1] = mixing[p]
    ends = [0, patches - 1]
    place = lambda ref: _Placed(ref, ends)
    edge_quads(odd_ref[0] == 1, patches, advance(states_ref, lambda p: mixing[p], place(new_ref)),
               w_ref, rw_ref, ow_ref, q_ref, qg_ref, far_ref, near_ref, sq_s, x_s)


class _Placed:
    def __init__(self, ref, items):
        self.ref, self.items = ref, items

    def __setitem__(self, where, value):
        self.ref[where[0], self.items.index(where[1])] = value


def advance_kernel(mix_ref, states_ref, w_ref, rw_ref, ow_ref, qe_ref, qge_ref, new_ref, *refs):
    *outs, sq_s, x_s, q_s = refs
    items = list(range(1, states_ref.shape[1] - 1))
    squash = advance(states_ref, lambda p: mix_ref[p - 1], _Placed(new_ref, items))
    inner_quads(items, squash, w_ref, rw_ref, ow_ref, qe_ref, qge_ref, outs, sq_s, x_s, q_s)


def last_kernel(*refs):
    *states, out_hbm, out_s, sems = refs[6:]
    mixing = [m.astype(BF16) for m in inverse_roots(*totals(refs[:6]))]
    slots, patches = out_s.shape[:2]
    copies = []
    for p in range(patches):
        for t in range(slots):
            if len(states) == 1:
                value = states[0][t, p]
            elif p in (0, patches - 1):
                value = states[0][t, min(p, 1)]
            else:
                value = states[1][t, p - 1]
            out_s[t, p] = dot_nt(value, mixing[p]).astype(BF16)
            copies.append(pltpu.make_async_copy(out_s.at[t, p], out_hbm.at[t, p], sems.at[len(copies)]))
            copies[-1].start()
    for c in copies:
        c.wait()


SPACES = {"s": pltpu.SMEM, "v": pltpu.VMEM, "h": pltpu.HBM}


def vmem_of(s):
    if isinstance(s, list):
        return tuple(vmem_of(e) for e in s)
    return pltpu.VMEM(*s) if isinstance(s, tuple) else s


def call(kernel, out_shape, args, kinds, scratch=(), flops=10 ** 9, out_kinds=None):
    outs = [jax.ShapeDtypeStruct(s, d) for s, d in out_shape]
    spec = lambda k: pl.BlockSpec(memory_space=SPACES[k])
    return pl.pallas_call(
        kernel,
        out_shape=outs,
        in_specs=[spec(k) for k in kinds],
        out_specs=[spec(k) for k in (out_kinds or "v" * len(outs))],
        scratch_shapes=[vmem_of(s) for s in scratch],
        cost_estimate=pl.CostEstimate(flops=flops, bytes_accessed=0, transcendentals=0),
        compiler_params=pltpu.CompilerParams(vmem_limit_bytes=VMEM_LIMIT),
        name=kernel.__name__,
    )(*args)


def neighbours(far, near):
    count = lax.axis_size("region")
    mate = [(r, r ^ 1) for r in range(count)]
    cross = [(r, (r + 1) % count if r % 2 else (r - 1) % count) for r in range(count)]
    return lax.ppermute(far, "region", cross), lax.ppermute(near, "region", mate)


def over_slots(msg):
    count = lax.axis_size("slot")
    if count == 2:
        return lax.ppermute(msg, "slot", [(0, 1), (1, 0)])
    mine = msg.astype(F32)
    return (lax.psum(mine, "slot") - mine).astype(BF16)


def shards(ensemble, observations, operator_weight, obs_precision, channel_mask):
    slots, patches, rows, members = ensemble.shape
    channels = operator_weight.shape[0]
    if lax.axis_size("region") % 2 or patches % 2 or not 4 <= patches <= 16:
        raise ValueError("unsupported split")
    inner = patches - 2
    odd = (lax.axis_index("region") % 2).astype(jnp.int32).reshape(1)
    edge = ((members + 16, members), BF16)
    gram = lambda n: ((n, members, members), F32)
    grad = lambda n: ((n, members), F32)
    message = lambda n: ((n // 2 * members + -(-(n // 2 + n) // 16) * 16, members), BF16)
    inner_out = [gram(inner), grad(inner), message(inner), gram(2), grad(2)]
    inner_scratch = (
        ((inner, rows, slots * members), BF16),
        [((inner, slots * channels, members), BF16), ((inner, members, slots * channels), BF16)],
        gram(inner),
    )
    scratch = lambda n: (
        ((n, rows, slots * members), BF16),
        [((n, slots * channels, members), BF16), ((n, members, slots * channels), BF16)],
    )
    rw = ((slots, channels, members), F32)
    ow = ((16, slots * channels), BF16)
    state = lambda n: ((slots, n, rows, members), BF16)
    prec = obs_precision[None, :]
    dma = pltpu.SemaphoreType.DMA
    hbm = lambda x: pltpu.with_memory_space_constraint(x, pltpu.HBM)

    states, weight, qe, qge, far, near, root_w, obs_w = call(
        first_kernel,
        [state(patches), (operator_weight.shape, BF16), gram(2), grad(2), edge, edge, rw, ow],
        (odd, hbm(ensemble), hbm(operator_weight), hbm(observations), hbm(prec), hbm(channel_mask)),
        "shhhhh",
        scratch(2) + (
            (observations.shape, F32),
            (prec.shape, F32),
            (channel_mask.shape, jnp.int32),
            dma((4 + slots * patches,)),
        ),
    )
    far, near = neighbours(far, near)
    *loc, msg, qi, qgi = call(
        inner_kernel, inner_out, (states, weight, root_w, obs_w, qe, qge), "vvvvvv", inner_scratch
    )
    parts = (states,)
    for step in range(OUTER):
        sums = tuple(
            call(sums_kernel, [gram(inner), grad(inner), grad(inner)], (*loc, over_slots(msg)), "vvv", flops=10 ** 8)
        )
        *loc, msg = call(
            combine_kernel,
            [gram(2), grad(2), message(2)],
            (odd, qe, qge, qi, qgi, far, near),
            "svvvvvv",
        )
        sums += (*loc, over_slots(msg))
        if step == OUTER - 1:
            break
        if len(parts) > 1:
            edges, inside = parts
            states = jnp.concatenate([edges[:, :1], inside, edges[:, 1:]], axis=1)
        mix, edges, qe, qge, far, near = call(
            root_kernel,
            [((inner, members, members), BF16), state(2), gram(2), grad(2), edge, edge],
            (odd, *sums, states, weight, root_w, obs_w),
            "s" + "v" * 10,
            scratch(2),
        )
        far, near = neighbours(far, near)
        inside, *loc, msg, qi, qgi = call(
            advance_kernel,
            [state(inner)] + inner_out,
            (mix, states, weight, root_w, obs_w, qe, qge),
            "vvvvvvv",
            inner_scratch,
        )
        parts = (edges, inside)
    return call(
        last_kernel,
        [state(patches)],
        sums + parts,
        "v" * (6 + len(parts)),
        (state(patches), dma((slots * patches,))),
        out_kinds="h",
    )[0]


def solution(mesh):
    return jax.shard_map(
        shards,
        mesh=mesh,
        in_specs=(
            P("slot", "region", None, None),
            P("slot", "region", None),
            P(),
            P(),
            P("slot", None),
        ),
        out_specs=P("slot", "region", None, None),
        check_vma=False,
    )
```

```python
import functools
import math

import jax
import jax.numpy as jnp
from jax import lax
from jax.experimental import pallas as pl
from jax.experimental.pallas import tpu as pltpu
from jax.sharding import PartitionSpec as P

OUTER = 2
NS_STEPS = 8
NS_SPLIT = 4
LOCAL_WEIGHT = 0.5
F32 = jnp.float32
BF16 = jnp.bfloat16
VMEM_LIMIT = 28 * 1024 * 1024


def dot(a, b):
    return lax.dot_general(a, b, (((1,), (0,)), ((), ())), preferred_element_type=F32)


def dot_nt(a, b):
    return lax.dot_general(a, b, (((1,), (1,)), ((), ())), preferred_element_type=F32)


def cat(parts, axis):
    return jnp.concatenate(parts, axis=axis)


def iotas(m):
    return (
        lax.broadcasted_iota(jnp.int32, (m, m), 0),
        lax.broadcasted_iota(jnp.int32, (m, m), 1),
    )


def prepare(obs_ref, prec_ref, mask_ref, rw_ref, ow_ref):
    slots, patches, channels = obs_ref.shape
    members = rw_ref.shape[-1]
    pad = ow_ref.shape[0] - patches
    for t in range(slots):
        weight = prec_ref[...] * mask_ref[t : t + 1, :].astype(F32) / OUTER
        root = jnp.sqrt(weight)
        rw_ref[t] = jnp.broadcast_to(root, (members, channels)).T
        rows = (obs_ref[t] * root).astype(F32)
        if pad:
            rows = cat([rows, jnp.zeros((pad, channels), F32)], 0)
        ow_ref[:, t * channels : (t + 1) * channels] = rows.astype(BF16)


def quads(items, squash, w_ref, rw_ref, ow_ref, store, sq_s, xs, before_a=None, before_b=None):
    slots, channels, members = rw_ref.shape
    x_s, xt_s = xs

    def stage_a(i):
        for t in range(slots):
            sq_s[i, :, t * members : (t + 1) * members] = squash(items[i], t)

    def stage_b(i):
        predicted = dot(w_ref[...], sq_s[i])
        for t in range(slots):
            part = predicted[:, t * members : (t + 1) * members]
            x = (part * rw_ref[t]).astype(BF16)
            x_s[i, t * channels : (t + 1) * channels, :] = x
            xt_s[i, :, t * channels : (t + 1) * channels] = x.T

    def stage_c(i):
        x = x_s[i]
        left = cat([xt_s[i], ow_ref[...]], 0)
        both = dot(left, x)
        square = both[:members]
        tail = both[members:]
        rows = lax.broadcasted_iota(jnp.int32, tail.shape, 0)
        inner = jnp.sum(jnp.where(rows == items[i], tail, 0.0), axis=0, keepdims=True)
        scale = 1.0 / members
        row = jnp.sum(square, axis=0, keepdims=True) * scale
        col = jnp.sum(square, axis=1, keepdims=True) * scale
        total = jnp.sum(row, axis=1, keepdims=True) * scale
        diff = inner - row
        grad = diff - jnp.sum(diff, axis=1, keepdims=True) * scale
        store(items[i], square - row - (col - total), grad)

    n = len(items)
    for i in range(n):
        if before_a is not None:
            before_a(i)
        stage_a(i)
    for i in range(n):
        if before_b is not None:
            before_b(i)
        stage_b(i)
    for i in range(n):
        stage_c(i)


def edges_of(odd, low, high, far_ref, near_ref):
    members = low[0].shape[0]
    pad = jnp.zeros((far_ref.shape[0] - members - 1, members), F32)
    low = cat([low[0], low[1], pad], 0)
    high = cat([high[0], high[1], pad], 0)
    far_ref[...] = jnp.where(odd, high, low).astype(BF16)
    near_ref[...] = jnp.where(odd, low, high).astype(BF16)


def mixed(v):
    return [v[p + 1] + LOCAL_WEIGHT * (v[p] + v[p + 2]) for p in range(len(v) - 2)]


def pack(grams, grads, out_ref):
    patches, members = len(grams), grams[0].shape[0]
    rid, cid = iotas(members)
    half = patches // 2
    rows = []
    for k in range(half):
        a, b = grams[k], grams[k + half]
        out_ref[k * members : (k + 1) * members] = jnp.where(rid <= cid, a, b).astype(BF16)
        rows.append(jnp.sum(jnp.where(rid == cid, b, 0.0), axis=0, keepdims=True))
    rows += list(grads)
    extra = out_ref.shape[0] - half * members
    rows.append(jnp.zeros((extra - len(rows), members), F32))
    out_ref[half * members :] = cat(rows, 0).astype(BF16)


def unpack(in_ref, patches):
    members = in_ref.shape[1]
    rid, cid = iotas(members)
    half = patches // 2
    rows = in_ref[half * members :].astype(F32)
    grams = [None] * patches
    for k in range(half):
        x = in_ref[k * members : (k + 1) * members].astype(F32)
        xt = x.T
        diag = rows[k : k + 1]
        grams[k] = jnp.where(rid <= cid, x, xt)
        grams[k + half] = jnp.where(rid > cid, x, jnp.where(rid < cid, xt, diag))
    return grams, [rows[half + p : half + p + 1] for p in range(patches)]


def inverse_roots(shifted, norm, grads):
    members = shifted[0].shape[0]
    every = range(len(shifted))
    rid, cid = iotas(members)
    identity = jnp.where(rid == cid, 1.0, 0.0).astype(F32)
    inv = [1.0 / v for v in norm]
    y = [jnp.broadcast_to(g, (8, members)) for g in grads]

    def tile(row):
        high = row.astype(BF16).astype(F32)
        return cat([high, row - high], 0).astype(BF16)

    def in_pairs(left, right):
        out = []
        for i in range(0, len(left), 2):
            zero = jnp.zeros_like(right[i])
            both = cat([cat([right[i], zero], 1), cat([zero, right[i + 1]], 1)], 0)
            prod = dot(cat(left[i : i + 2], 1), both)
            out += [prod[:, :members], prod[:, members:]]
        return out

    def times(right, parts):
        prod = in_pairs([cat(rows, 0) for rows in zip(*parts)], right)
        at, found = 0, []
        for part in parts:
            size = part[0].shape[0]
            found.append([v[at : at + size] for v in prod])
            at += size
        return found

    z = [None for _ in every]
    for step in range(NS_SPLIT):
        rows = [tile(v) for v in y]
        if step == 0:
            th = [v.astype(BF16) for v in shifted]
            square, row = times(th, [th, rows])
            t = [shifted[i] * inv[i] for i in every]
            square = [square[i] * (inv[i] * inv[i]) for i in every]
            row = [row[i] * inv[i] for i in every]
            z = [1.5 * identity - 0.5 * v for v in t]
        else:
            th = [v.astype(BF16) for v in t]
            square, row, moved = times(th, [th, rows, [v.astype(BF16) for v in z]])
            z = [1.5 * z[i] - 0.5 * moved[i] for i in every]
        y = [1.5 * y[i] - 0.5 * (row[i][:8] + row[i][8:]) for i in every]
        shrunk = in_pairs([(1.5 * t[i] - 0.25 * square[i]).astype(BF16) for i in every], th)
        if step == 0:
            shrunk = [shrunk[i] * inv[i] for i in every]
        t = [2.25 * t[i] - shrunk[i] for i in every]
    d = [identity - v for v in t]
    for step in range(NS_SPLIT, NS_STEPS):
        dh = [v.astype(BF16) for v in d]
        rows = [tile(v) for v in y]
        zh = [v.astype(BF16) for v in z]
        if step < NS_STEPS - 1:
            square, row, moved = times(dh, [dh, rows, zh])
            cube = in_pairs([v.astype(BF16) for v in square], dh)
            d = [0.75 * square[i] + 0.25 * cube[i] for i in every]
        else:
            row, moved = times(dh, [rows, zh])
        z = [z[i] + 0.5 * moved[i] for i in every]
        y = [y[i] + 0.5 * (row[i][:8] + row[i][8:]) for i in every]

    scale = math.sqrt(members - 1.0)
    share = 1.0 / members
    out = []
    for i in every:
        yn = y[i] * (1.0 / norm[i])
        high = yn.astype(BF16).astype(F32)
        rows = dot(cat([high, yn - high], 0).astype(BF16), z[i].astype(BF16))
        along = (rows[:8] + rows[8:])[0:1]
        row = jnp.sum(z[i], axis=0, keepdims=True) * share
        col = jnp.sum(z[i], axis=1, keepdims=True) * share
        level = jnp.sum(yn[0:1] * row, axis=1, keepdims=True)
        out.append((z[i] - col) * (scale / jnp.sqrt(norm[i])) + (along - level + share))
    return out


def squash_of(states_ref):
    return lambda p, t: jnp.tanh(states_ref[t, p].astype(F32)).astype(BF16)


def move(parts, mixing):
    moved = dot_nt(cat(parts, 0), mixing).astype(BF16)
    rows = parts[0].shape[0]
    return [moved[k * rows : (k + 1) * rows] for k in range(len(parts))]


def advance(states_ref, mixing_of, new_ref):
    slots = states_ref.shape[0]
    fresh = {}

    def squash(p, t):
        if p not in fresh:
            fresh[p] = move([states_ref[k, p] for k in range(slots)], mixing_of(p))
        new_ref[t, p] = fresh[p][t]
        return jnp.tanh(fresh[p][t].astype(F32)).astype(BF16)

    return squash


def into(q_ref, qg_ref, first):
    def store(p, gram, grad):
        q_ref[p - first] = gram
        qg_ref[p - first : p - first + 1] = grad

    return store


def edge_quads(odd, patches, squash, w_ref, rw_ref, ow_ref, q_ref, qg_ref, far_ref, near_ref, sq_s, x_s,
               **hooks):
    ends = [0, patches - 1]
    found = {}

    def store(p, gram, grad):
        found[p] = (gram, grad)
        k = ends.index(p)
        q_ref[k] = gram
        qg_ref[k : k + 1] = grad

    quads(ends, squash, w_ref, rw_ref, ow_ref, store, sq_s, x_s, **hooks)
    edges_of(odd, found[ends[0]], found[ends[1]], far_ref, near_ref)


def first_kernel(odd_ref, states_hbm, w_hbm, obs_hbm, prec_hbm, mask_hbm,
                 states_ref, w_ref, q_ref, qg_ref, far_ref, near_ref, rw_ref, ow_ref,
                 sq_s, x_s, obs_s, prec_s, mask_s, sems):
    patches = states_ref.shape[1]
    slots = states_ref.shape[0]
    ends = [0, patches - 1]
    small = [
        pltpu.make_async_copy(prec_hbm, prec_s, sems.at[0]),
        pltpu.make_async_copy(mask_hbm, mask_s, sems.at[1]),
        pltpu.make_async_copy(obs_hbm, obs_s, sems.at[2]),
    ]
    weights = pltpu.make_async_copy(w_hbm, w_ref, sems.at[3])
    state = {
        (t, p): pltpu.make_async_copy(
            states_hbm.at[t, p], states_ref.at[t, p], sems.at[4 + t * patches + p]
        )
        for p in range(patches)
        for t in range(slots)
    }
    for c in small:
        c.start()
    for p in ends:
        for t in range(slots):
            state[t, p].start()
    weights.start()
    late = [state[t, p] for p in range(1, patches - 1) for t in range(slots)]

    def before_a(i):
        for t in range(slots):
            state[t, ends[i]].wait()
        if i == 0:
            for c in late:
                c.start()

    def before_b(i):
        if i == 0:
            for c in small:
                c.wait()
            prepare(obs_s, prec_s, mask_s, rw_ref, ow_ref)
            weights.wait()

    edge_quads(odd_ref[0] == 1, patches, squash_of(states_ref), w_ref, rw_ref, ow_ref,
               q_ref, qg_ref, far_ref, near_ref, sq_s, x_s, before_a=before_a, before_b=before_b)
    for c in late:
        c.wait()


def finish_inner(qe_ref, qge_ref, found, outs):
    loc_ref, locg_ref, msg_ref, q_ref, qg_ref = outs
    inner = len(found)
    grams = mixed([qe_ref[0]] + [found[p][0][...] for p in range(inner)] + [qe_ref[1]])
    grads = mixed([qge_ref[0:1]] + [found[p][1] for p in range(inner)] + [qge_ref[1:2]])
    for p in range(inner):
        loc_ref[p] = grams[p]
        locg_ref[p : p + 1] = grads[p]
    pack(grams, grads, msg_ref)
    for k, p in enumerate((0, inner - 1)):
        q_ref[k] = found[p][0][...]
        qg_ref[k : k + 1] = found[p][1]


def inner_quads(items, squash, w_ref, rw_ref, ow_ref, qe_ref, qge_ref, outs, sq_s, x_s, q_s):
    found = []

    def store(p, gram, grad):
        q_s[len(found)] = gram
        found.append((q_s.at[len(found)], grad))

    quads(items, squash, w_ref, rw_ref, ow_ref, store, sq_s, x_s)
    finish_inner(qe_ref, qge_ref, found, outs)


def inner_kernel(states_ref, w_ref, rw_ref, ow_ref, qe_ref, qge_ref, *refs):
    *outs, sq_s, x_s, q_s = refs
    items = list(range(1, states_ref.shape[1] - 1))
    inner_quads(items, squash_of(states_ref), w_ref, rw_ref, ow_ref, qe_ref, qge_ref, outs, sq_s, x_s, q_s)


def combine_kernel(odd_ref, qe_ref, qge_ref, qi_ref, qgi_ref, far_ref, near_ref, loc_ref, locg_ref, msg_ref):
    odd = odd_ref[0] == 1
    members = qe_ref.shape[-1]
    far = far_ref[...].astype(F32)
    near = near_ref[...].astype(F32)
    left = jnp.where(odd, near, far)
    right = jnp.where(odd, far, near)
    tail = slice(members, members + 1)
    grams = mixed([left[:members], qe_ref[0], qi_ref[0]]) + mixed([qi_ref[1], qe_ref[1], right[:members]])
    grads = mixed([left[tail], qge_ref[0:1], qgi_ref[0:1]]) + mixed([qgi_ref[1:2], qge_ref[1:2], right[tail]])
    for k in range(2):
        loc_ref[k] = grams[k]
        locg_ref[k : k + 1] = grads[k]
    pack(grams, grads, msg_ref)


def shifted_sums(loc_ref, locg_ref, msg_ref):
    n, members = loc_ref.shape[:2]
    rid, cid = iotas(members)
    shift = jnp.where(rid == cid, members - 1.0, 0.0).astype(F32)
    grams, grads = unpack(msg_ref, n)
    shifted = [loc_ref[p] + grams[p] + shift for p in range(n)]
    square = [jnp.sum(jnp.sum(s * s, axis=0, keepdims=True), axis=1, keepdims=True) for s in shifted]
    return shifted, [jnp.sqrt(s) for s in square], [locg_ref[p : p + 1] + grads[p] for p in range(n)]


def sums_kernel(loc_ref, locg_ref, msg_ref, shifted_ref, norm_ref, grad_ref):
    shifted, norm, grads = shifted_sums(loc_ref, locg_ref, msg_ref)
    for p in range(len(grads)):
        shifted_ref[p] = shifted[p]
        norm_ref[p : p + 1] = jnp.broadcast_to(norm[p], grads[p].shape)
        grad_ref[p : p + 1] = grads[p]


def totals(refs):
    shifted_ref, norm_ref, grad_ref = refs[:3]
    shifted, norm, grads = shifted_sums(*refs[3:])
    n = shifted_ref.shape[0]
    return (
        shifted[:1] + [shifted_ref[p] for p in range(n)] + shifted[1:],
        norm[:1] + [norm_ref[p : p + 1, 0:1] for p in range(n)] + norm[1:],
        grads[:1] + [grad_ref[p : p + 1] for p in range(n)] + grads[1:],
    )


def root_kernel(odd_ref, *refs):
    sums, (states_ref, w_ref, rw_ref, ow_ref, mix_ref, new_ref, q_ref, qg_ref, far_ref, near_ref, sq_s, x_s) = (
        refs[:6],
        refs[6:],
    )
    mixing = [m.astype(BF16) for m in inverse_roots(*totals(sums))]
    patches = states_ref.shape[1]
    for p in range(1, patches - 1):
        mix_ref[p - 1] = mixing[p]
    ends = [0, patches - 1]
    place = lambda ref: _Placed(ref, ends)
    edge_quads(odd_ref[0] == 1, patches, advance(states_ref, lambda p: mixing[p], place(new_ref)),
               w_ref, rw_ref, ow_ref, q_ref, qg_ref, far_ref, near_ref, sq_s, x_s)


class _Placed:
    def __init__(self, ref, items):
        self.ref, self.items = ref, items

    def __setitem__(self, where, value):
        self.ref[where[0], self.items.index(where[1])] = value


def advance_kernel(mix_ref, states_ref, w_ref, rw_ref, ow_ref, qe_ref, qge_ref, new_ref, *refs):
    *outs, sq_s, x_s, q_s = refs
    items = list(range(1, states_ref.shape[1] - 1))
    squash = advance(states_ref, lambda p: mix_ref[p - 1], _Placed(new_ref, items))
    inner_quads(items, squash, w_ref, rw_ref, ow_ref, qe_ref, qge_ref, outs, sq_s, x_s, q_s)


def last_kernel(*refs):
    *states, out_hbm, out_s, sems = refs[6:]
    mixing = [m.astype(BF16) for m in inverse_roots(*totals(refs[:6]))]
    slots, patches = out_s.shape[:2]
    copies = []

    def value(t, p):
        if len(states) == 1:
            return states[0][t, p]
        if p in (0, patches - 1):
            return states[0][t, min(p, 1)]
        return states[1][t, p - 1]

    for p in range(patches):
        for t, fresh in enumerate(move([value(t, p) for t in range(slots)], mixing[p])):
            out_s[t, p] = fresh
            copies.append(pltpu.make_async_copy(out_s.at[t, p], out_hbm.at[t, p], sems.at[len(copies)]))
            copies[-1].start()
    for c in copies:
        c.wait()


SPACES = {"s": pltpu.SMEM, "v": pltpu.VMEM, "h": pltpu.HBM}


def vmem_of(s):
    if isinstance(s, list):
        return tuple(vmem_of(e) for e in s)
    return pltpu.VMEM(*s) if isinstance(s, tuple) else s


def call(kernel, out_shape, args, kinds, scratch=(), flops=10 ** 9, out_kinds=None):
    outs = [jax.ShapeDtypeStruct(s, d) for s, d in out_shape]
    spec = lambda k: pl.BlockSpec(memory_space=SPACES[k])
    return pl.pallas_call(
        kernel,
        out_shape=outs,
        in_specs=[spec(k) for k in kinds],
        out_specs=[spec(k) for k in (out_kinds or "v" * len(outs))],
        scratch_shapes=[vmem_of(s) for s in scratch],
        cost_estimate=pl.CostEstimate(flops=flops, bytes_accessed=0, transcendentals=0),
        compiler_params=pltpu.CompilerParams(vmem_limit_bytes=VMEM_LIMIT),
        name=kernel.__name__,
    )(*args)


def neighbours(far, near):
    count = lax.axis_size("region")
    mate = [(r, r ^ 1) for r in range(count)]
    cross = [(r, (r + 1) % count if r % 2 else (r - 1) % count) for r in range(count)]
    return lax.ppermute(far, "region", cross), lax.ppermute(near, "region", mate)


def over_slots(msg):
    count = lax.axis_size("slot")
    if count == 2:
        return lax.ppermute(msg, "slot", [(0, 1), (1, 0)])
    mine = msg.astype(F32)
    return (lax.psum(mine, "slot") - mine).astype(BF16)


def shards(ensemble, observations, operator_weight, obs_precision, channel_mask):
    slots, patches, rows, members = ensemble.shape
    channels = operator_weight.shape[0]
    if lax.axis_size("region") % 2 or patches % 2 or not 4 <= patches <= 16:
        raise ValueError("unsupported split")
    inner = patches - 2
    odd = (lax.axis_index("region") % 2).astype(jnp.int32).reshape(1)
    edge = ((members + 16, members), BF16)
    gram = lambda n: ((n, members, members), F32)
    grad = lambda n: ((n, members), F32)
    message = lambda n: ((n // 2 * members + -(-(n // 2 + n) // 16) * 16, members), BF16)
    inner_out = [gram(inner), grad(inner), message(inner), gram(2), grad(2)]
    inner_scratch = (
        ((inner, rows, slots * members), BF16),
        [((inner, slots * channels, members), BF16), ((inner, members, slots * channels), BF16)],
        gram(inner),
    )
    scratch = lambda n: (
        ((n, rows, slots * members), BF16),
        [((n, slots * channels, members), BF16), ((n, members, slots * channels), BF16)],
    )
    rw = ((slots, channels, members), F32)
    ow = ((16, slots * channels), BF16)
    state = lambda n: ((slots, n, rows, members), BF16)
    prec = obs_precision[None, :]
    dma = pltpu.SemaphoreType.DMA
    hbm = lambda x: pltpu.with_memory_space_constraint(x, pltpu.HBM)

    states, weight, qe, qge, far, near, root_w, obs_w = call(
        first_kernel,
        [state(patches), (operator_weight.shape, BF16), gram(2), grad(2), edge, edge, rw, ow],
        (odd, hbm(ensemble), hbm(operator_weight), hbm(observations), hbm(prec), hbm(channel_mask)),
        "shhhhh",
        scratch(2) + (
            (observations.shape, F32),
            (prec.shape, F32),
            (channel_mask.shape, jnp.int32),
            dma((4 + slots * patches,)),
        ),
    )
    far, near = neighbours(far, near)
    *loc, msg, qi, qgi = call(
        inner_kernel, inner_out, (states, weight, root_w, obs_w, qe, qge), "vvvvvv", inner_scratch
    )
    parts = (states,)
    for step in range(OUTER):
        sums = tuple(
            call(sums_kernel, [gram(inner), grad(inner), grad(inner)], (*loc, over_slots(msg)), "vvv", flops=10 ** 8)
        )
        *loc, msg = call(
            combine_kernel,
            [gram(2), grad(2), message(2)],
            (odd, qe, qge, qi, qgi, far, near),
            "svvvvvv",
        )
        sums += (*loc, over_slots(msg))
        if step == OUTER - 1:
            break
        if len(parts) > 1:
            edges, inside = parts
            states = jnp.concatenate([edges[:, :1], inside, edges[:, 1:]], axis=1)
        mix, edges, qe, qge, far, near = call(
            root_kernel,
            [((inner, members, members), BF16), state(2), gram(2), grad(2), edge, edge],
            (odd, *sums, states, weight, root_w, obs_w),
            "s" + "v" * 10,
            scratch(2),
        )
        far, near = neighbours(far, near)
        inside, *loc, msg, qi, qgi = call(
            advance_kernel,
            [state(inner)] + inner_out,
            (mix, states, weight, root_w, obs_w, qe, qge),
            "vvvvvvv",
            inner_scratch,
        )
        parts = (edges, inside)
    return call(
        last_kernel,
        [state(patches)],
        sums + parts,
        "v" * (6 + len(parts)),
        (state(patches), dma((slots * patches,))),
        out_kinds="h",
    )[0]


def solution(mesh):
    return jax.shard_map(
        shards,
        mesh=mesh,
        in_specs=(
            P("slot", "region", None, None),
            P("slot", "region", None),
            P(),
            P(),
            P("slot", None),
        ),
        out_specs=P("slot", "region", None, None),
        check_vma=False,
    )
```

```python
import functools
import math

import jax
import jax.numpy as jnp
from jax import lax
from jax.experimental import pallas as pl
from jax.experimental.pallas import tpu as pltpu
from jax.sharding import PartitionSpec as P

OUTER = 2
NS_STEPS = 8
NS_SPLIT = 4
LOCAL_WEIGHT = 0.5
F32 = jnp.float32
BF16 = jnp.bfloat16
VMEM_LIMIT = 28 * 1024 * 1024


def dot(a, b):
    return lax.dot_general(a, b, (((1,), (0,)), ((), ())), preferred_element_type=F32)


def dot_nt(a, b):
    return lax.dot_general(a, b, (((1,), (1,)), ((), ())), preferred_element_type=F32)


def cat(parts, axis):
    return jnp.concatenate(parts, axis=axis)


def iotas(m):
    return (
        lax.broadcasted_iota(jnp.int32, (m, m), 0),
        lax.broadcasted_iota(jnp.int32, (m, m), 1),
    )


def prepare(obs_ref, prec_ref, mask_ref, rw_ref, ow_ref):
    slots, patches, channels = obs_ref.shape
    members = rw_ref.shape[-1]
    pad = ow_ref.shape[0] - patches
    for t in range(slots):
        weight = prec_ref[...] * mask_ref[t : t + 1, :].astype(F32) / OUTER
        root = jnp.sqrt(weight)
        rw_ref[t] = jnp.broadcast_to(root, (members, channels)).T
        rows = (obs_ref[t] * root).astype(F32)
        if pad:
            rows = cat([rows, jnp.zeros((pad, channels), F32)], 0)
        ow_ref[:, t * channels : (t + 1) * channels] = rows.astype(BF16)


def quads(items, squash, w_ref, rw_ref, ow_ref, store, sq_s, xs, before_a=None, before_b=None):
    slots, channels, members = rw_ref.shape
    x_s, xt_s = xs

    def stage_a(i):
        for t in range(slots):
            sq_s[i, :, t * members : (t + 1) * members] = squash(items[i], t)

    def stage_b(i):
        predicted = dot(w_ref[...], sq_s[i])
        for t in range(slots):
            part = predicted[:, t * members : (t + 1) * members]
            x = (part * rw_ref[t]).astype(BF16)
            x_s[i, t * channels : (t + 1) * channels, :] = x
            xt_s[i, :, t * channels : (t + 1) * channels] = x.T

    def stage_c(i):
        x = x_s[i]
        left = cat([xt_s[i], ow_ref[...]], 0)
        both = dot(left, x)
        square = both[:members]
        tail = both[members:]
        rows = lax.broadcasted_iota(jnp.int32, tail.shape, 0)
        inner = jnp.sum(jnp.where(rows == items[i], tail, 0.0), axis=0, keepdims=True)
        scale = 1.0 / members
        row = jnp.sum(square, axis=0, keepdims=True) * scale
        col = jnp.sum(square, axis=1, keepdims=True) * scale
        total = jnp.sum(row, axis=1, keepdims=True) * scale
        diff = inner - row
        grad = diff - jnp.sum(diff, axis=1, keepdims=True) * scale
        store(items[i], square - row - (col - total), grad)

    n = len(items)
    for i in range(n):
        if before_a is not None:
            before_a(i)
        stage_a(i)
    for i in range(n):
        if before_b is not None:
            before_b(i)
        stage_b(i)
    for i in range(n):
        stage_c(i)


def edges_of(odd, low, high, far_ref, near_ref):
    members = low[0].shape[0]
    pad = jnp.zeros((far_ref.shape[0] - members - 1, members), F32)
    low = cat([low[0], low[1], pad], 0)
    high = cat([high[0], high[1], pad], 0)
    far_ref[...] = jnp.where(odd, high, low).astype(BF16)
    near_ref[...] = jnp.where(odd, low, high).astype(BF16)


def mixed(v):
    return [v[p + 1] + LOCAL_WEIGHT * (v[p] + v[p + 2]) for p in range(len(v) - 2)]


def pack(grams, grads, out_ref):
    patches, members = len(grams), grams[0].shape[0]
    rid, cid = iotas(members)
    half = patches // 2
    rows = []
    for k in range(half):
        a, b = grams[k], grams[k + half]
        out_ref[k * members : (k + 1) * members] = jnp.where(rid <= cid, a, b).astype(BF16)
        rows.append(jnp.sum(jnp.where(rid == cid, b, 0.0), axis=0, keepdims=True))
    rows += list(grads)
    extra = out_ref.shape[0] - half * members
    rows.append(jnp.zeros((extra - len(rows), members), F32))
    out_ref[half * members :] = cat(rows, 0).astype(BF16)


def unpack(in_ref, patches):
    members = in_ref.shape[1]
    rid, cid = iotas(members)
    half = patches // 2
    rows = in_ref[half * members :].astype(F32)
    grams = [None] * patches
    for k in range(half):
        x = in_ref[k * members : (k + 1) * members].astype(F32)
        xt = x.T
        diag = rows[k : k + 1]
        grams[k] = jnp.where(rid <= cid, x, xt)
        grams[k + half] = jnp.where(rid > cid, x, jnp.where(rid < cid, xt, diag))
    return grams, [rows[half + p : half + p + 1] for p in range(patches)]


def inverse_roots(shifted, norm, grads):
    members = shifted[0].shape[0]
    every = range(len(shifted))
    rid, cid = iotas(members)
    identity = jnp.where(rid == cid, 1.0, 0.0).astype(F32)
    inv = [1.0 / v for v in norm]
    y = [jnp.broadcast_to(g, (8, members)) for g in grads]

    def tile(row):
        high = row.astype(BF16).astype(F32)
        return cat([high, row - high], 0).astype(BF16)

    def in_pairs(left, right):
        out = []
        for i in range(0, len(left), 2):
            zero = jnp.zeros_like(right[i])
            both = cat([cat([right[i], zero], 1), cat([zero, right[i + 1]], 1)], 0)
            prod = dot(cat(left[i : i + 2], 1), both)
            out += [prod[:, :members], prod[:, members:]]
        return out

    def times(right, parts):
        prod = in_pairs([cat(rows, 0) for rows in zip(*parts)], right)
        at, found = 0, []
        for part in parts:
            size = part[0].shape[0]
            found.append([v[at : at + size] for v in prod])
            at += size
        return found

    z = [None for _ in every]
    for step in range(NS_SPLIT):
        rows = [tile(v) for v in y]
        if step == 0:
            th = [v.astype(BF16) for v in shifted]
            square = in_pairs(th, th)
            (row,) = times(th, [rows])
            t = [shifted[i] * inv[i] for i in every]
            square = [square[i] * (inv[i] * inv[i]) for i in every]
            row = [row[i] * inv[i] for i in every]
            z = [1.5 * identity - 0.5 * v for v in t]
        else:
            th = [v.astype(BF16) for v in t]
            square = in_pairs(th, th)
        shrunk = in_pairs([(1.5 * t[i] - 0.25 * square[i]).astype(BF16) for i in every], th)
        if step:
            row, moved = times(th, [rows, [v.astype(BF16) for v in z]])
            z = [1.5 * z[i] - 0.5 * moved[i] for i in every]
        y = [1.5 * y[i] - 0.5 * (row[i][:8] + row[i][8:]) for i in every]
        if step == 0:
            shrunk = [shrunk[i] * inv[i] for i in every]
        t = [2.25 * t[i] - shrunk[i] for i in every]
    d = [identity - v for v in t]
    for step in range(NS_SPLIT, NS_STEPS):
        dh = [v.astype(BF16) for v in d]
        rows = [tile(v) for v in y]
        zh = [v.astype(BF16) for v in z]
        if step < NS_STEPS - 1:
            square = in_pairs(dh, dh)
            cube = in_pairs([v.astype(BF16) for v in square], dh)
            row, moved = times(dh, [rows, zh])
            d = [0.75 * square[i] + 0.25 * cube[i] for i in every]
        else:
            row, moved = times(dh, [rows, zh])
        z = [z[i] + 0.5 * moved[i] for i in every]
        y = [y[i] + 0.5 * (row[i][:8] + row[i][8:]) for i in every]

    scale = math.sqrt(members - 1.0)
    share = 1.0 / members
    out = []
    for i in every:
        yn = y[i] * (1.0 / norm[i])
        high = yn.astype(BF16).astype(F32)
        rows = dot(cat([high, yn - high], 0).astype(BF16), z[i].astype(BF16))
        along = (rows[:8] + rows[8:])[0:1]
        row = jnp.sum(z[i], axis=0, keepdims=True) * share
        col = jnp.sum(z[i], axis=1, keepdims=True) * share
        level = jnp.sum(yn[0:1] * row, axis=1, keepdims=True)
        out.append((z[i] - col) * (scale / jnp.sqrt(norm[i])) + (along - level + share))
    return out


def squash_of(states_ref):
    return lambda p, t: jnp.tanh(states_ref[t, p].astype(F32)).astype(BF16)


def move(parts, mixing):
    moved = dot_nt(cat(parts, 0), mixing).astype(BF16)
    rows = parts[0].shape[0]
    return [moved[k * rows : (k + 1) * rows] for k in range(len(parts))]


def advance(states_ref, mixing_of, new_ref):
    slots = states_ref.shape[0]
    fresh = {}

    def squash(p, t):
        if p not in fresh:
            fresh[p] = move([states_ref[k, p] for k in range(slots)], mixing_of(p))
        new_ref[t, p] = fresh[p][t]
        return jnp.tanh(fresh[p][t].astype(F32)).astype(BF16)

    return squash


def into(q_ref, qg_ref, first):
    def store(p, gram, grad):
        q_ref[p - first] = gram
        qg_ref[p - first : p - first + 1] = grad

    return store


def edge_quads(odd, patches, squash, w_ref, rw_ref, ow_ref, q_ref, qg_ref, far_ref, near_ref, sq_s, x_s,
               **hooks):
    ends = [0, patches - 1]
    found = {}

    def store(p, gram, grad):
        found[p] = (gram, grad)
        k = ends.index(p)
        q_ref[k] = gram
        qg_ref[k : k + 1] = grad

    quads(ends, squash, w_ref, rw_ref, ow_ref, store, sq_s, x_s, **hooks)
    edges_of(odd, found[ends[0]], found[ends[1]], far_ref, near_ref)


def first_kernel(odd_ref, states_hbm, w_hbm, obs_hbm, prec_hbm, mask_hbm,
                 states_ref, w_ref, q_ref, qg_ref, far_ref, near_ref, rw_ref, ow_ref,
                 sq_s, x_s, obs_s, prec_s, mask_s, sems):
    patches = states_ref.shape[1]
    slots = states_ref.shape[0]
    ends = [0, patches - 1]
    small = [
        pltpu.make_async_copy(prec_hbm, prec_s, sems.at[0]),
        pltpu.make_async_copy(mask_hbm, mask_s, sems.at[1]),
        pltpu.make_async_copy(obs_hbm, obs_s, sems.at[2]),
    ]
    weights = pltpu.make_async_copy(w_hbm, w_ref, sems.at[3])
    state = {
        (t, p): pltpu.make_async_copy(
            states_hbm.at[t, p], states_ref.at[t, p], sems.at[4 + t * patches + p]
        )
        for p in range(patches)
        for t in range(slots)
    }
    for c in small:
        c.start()
    for p in ends:
        for t in range(slots):
            state[t, p].start()
    weights.start()
    late = [state[t, p] for p in range(1, patches - 1) for t in range(slots)]

    def before_a(i):
        for t in range(slots):
            state[t, ends[i]].wait()
        if i == 0:
            for c in late:
                c.start()

    def before_b(i):
        if i == 0:
            for c in small:
                c.wait()
            prepare(obs_s, prec_s, mask_s, rw_ref, ow_ref)
            weights.wait()

    edge_quads(odd_ref[0] == 1, patches, squash_of(states_ref), w_ref, rw_ref, ow_ref,
               q_ref, qg_ref, far_ref, near_ref, sq_s, x_s, before_a=before_a, before_b=before_b)
    for c in late:
        c.wait()


def finish_inner(qe_ref, qge_ref, found, outs):
    loc_ref, locg_ref, msg_ref, q_ref, qg_ref = outs
    inner = len(found)
    grams = mixed([qe_ref[0]] + [found[p][0][...] for p in range(inner)] + [qe_ref[1]])
    grads = mixed([qge_ref[0:1]] + [found[p][1] for p in range(inner)] + [qge_ref[1:2]])
    for p in range(inner):
        loc_ref[p] = grams[p]
        locg_ref[p : p + 1] = grads[p]
    pack(grams, grads, msg_ref)
    for k, p in enumerate((0, inner - 1)):
        q_ref[k] = found[p][0][...]
        qg_ref[k : k + 1] = found[p][1]


def inner_quads(items, squash, w_ref, rw_ref, ow_ref, qe_ref, qge_ref, outs, sq_s, x_s, q_s):
    found = []

    def store(p, gram, grad):
        q_s[len(found)] = gram
        found.append((q_s.at[len(found)], grad))

    quads(items, squash, w_ref, rw_ref, ow_ref, store, sq_s, x_s)
    finish_inner(qe_ref, qge_ref, found, outs)


def inner_kernel(states_ref, w_ref, rw_ref, ow_ref, qe_ref, qge_ref, *refs):
    *outs, sq_s, x_s, q_s = refs
    items = list(range(1, states_ref.shape[1] - 1))
    inner_quads(items, squash_of(states_ref), w_ref, rw_ref, ow_ref, qe_ref, qge_ref, outs, sq_s, x_s, q_s)


def combine_kernel(odd_ref, qe_ref, qge_ref, qi_ref, qgi_ref, far_ref, near_ref, loc_ref, locg_ref, msg_ref):
    odd = odd_ref[0] == 1
    members = qe_ref.shape[-1]
    far = far_ref[...].astype(F32)
    near = near_ref[...].astype(F32)
    left = jnp.where(odd, near, far)
    right = jnp.where(odd, far, near)
    tail = slice(members, members + 1)
    grams = mixed([left[:members], qe_ref[0], qi_ref[0]]) + mixed([qi_ref[1], qe_ref[1], right[:members]])
    grads = mixed([left[tail], qge_ref[0:1], qgi_ref[0:1]]) + mixed([qgi_ref[1:2], qge_ref[1:2], right[tail]])
    for k in range(2):
        loc_ref[k] = grams[k]
        locg_ref[k : k + 1] = grads[k]
    pack(grams, grads, msg_ref)


def shifted_sums(loc_ref, locg_ref, msg_ref):
    n, members = loc_ref.shape[:2]
    rid, cid = iotas(members)
    shift = jnp.where(rid == cid, members - 1.0, 0.0).astype(F32)
    grams, grads = unpack(msg_ref, n)
    shifted = [loc_ref[p] + grams[p] + shift for p in range(n)]
    square = [jnp.sum(jnp.sum(s * s, axis=0, keepdims=True), axis=1, keepdims=True) for s in shifted]
    return shifted, [jnp.sqrt(s) for s in square], [locg_ref[p : p + 1] + grads[p] for p in range(n)]


def sums_kernel(loc_ref, locg_ref, msg_ref, shifted_ref, norm_ref, grad_ref):
    shifted, norm, grads = shifted_sums(loc_ref, locg_ref, msg_ref)
    for p in range(len(grads)):
        shifted_ref[p] = shifted[p]
        norm_ref[p : p + 1] = jnp.broadcast_to(norm[p], grads[p].shape)
        grad_ref[p : p + 1] = grads[p]


def totals(refs):
    shifted_ref, norm_ref, grad_ref = refs[:3]
    shifted, norm, grads = shifted_sums(*refs[3:])
    n = shifted_ref.shape[0]
    return (
        shifted[:1] + [shifted_ref[p] for p in range(n)] + shifted[1:],
        norm[:1] + [norm_ref[p : p + 1, 0:1] for p in range(n)] + norm[1:],
        grads[:1] + [grad_ref[p : p + 1] for p in range(n)] + grads[1:],
    )


def root_kernel(odd_ref, *refs):
    sums, (states_ref, w_ref, rw_ref, ow_ref, mix_ref, new_ref, q_ref, qg_ref, far_ref, near_ref, sq_s, x_s) = (
        refs[:6],
        refs[6:],
    )
    mixing = [m.astype(BF16) for m in inverse_roots(*totals(sums))]
    patches = states_ref.shape[1]
    for p in range(1, patches - 1):
        mix_ref[p - 1] = mixing[p]
    ends = [0, patches - 1]
    place = lambda ref: _Placed(ref, ends)
    edge_quads(odd_ref[0] == 1, patches, advance(states_ref, lambda p: mixing[p], place(new_ref)),
               w_ref, rw_ref, ow_ref, q_ref, qg_ref, far_ref, near_ref, sq_s, x_s)


class _Placed:
    def __init__(self, ref, items):
        self.ref, self.items = ref, items

    def __setitem__(self, where, value):
        self.ref[where[0], self.items.index(where[1])] = value


def advance_kernel(mix_ref, states_ref, w_ref, rw_ref, ow_ref, qe_ref, qge_ref, new_ref, *refs):
    *outs, sq_s, x_s, q_s = refs
    items = list(range(1, states_ref.shape[1] - 1))
    squash = advance(states_ref, lambda p: mix_ref[p - 1], _Placed(new_ref, items))
    inner_quads(items, squash, w_ref, rw_ref, ow_ref, qe_ref, qge_ref, outs, sq_s, x_s, q_s)


def last_kernel(*refs):
    *states, out_hbm, out_s, sems = refs[6:]
    mixing = [m.astype(BF16) for m in inverse_roots(*totals(refs[:6]))]
    slots, patches = out_s.shape[:2]
    copies = []

    def value(t, p):
        if len(states) == 1:
            return states[0][t, p]
        if p in (0, patches - 1):
            return states[0][t, min(p, 1)]
        return states[1][t, p - 1]

    for p in range(patches):
        for t, fresh in enumerate(move([value(t, p) for t in range(slots)], mixing[p])):
            out_s[t, p] = fresh
            copies.append(pltpu.make_async_copy(out_s.at[t, p], out_hbm.at[t, p], sems.at[len(copies)]))
            copies[-1].start()
    for c in copies:
        c.wait()


SPACES = {"s": pltpu.SMEM, "v": pltpu.VMEM, "h": pltpu.HBM}


def vmem_of(s):
    if isinstance(s, list):
        return tuple(vmem_of(e) for e in s)
    return pltpu.VMEM(*s) if isinstance(s, tuple) else s


def call(kernel, out_shape, args, kinds, scratch=(), flops=10 ** 9, out_kinds=None):
    outs = [jax.ShapeDtypeStruct(s, d) for s, d in out_shape]
    spec = lambda k: pl.BlockSpec(memory_space=SPACES[k])
    return pl.pallas_call(
        kernel,
        out_shape=outs,
        in_specs=[spec(k) for k in kinds],
        out_specs=[spec(k) for k in (out_kinds or "v" * len(outs))],
        scratch_shapes=[vmem_of(s) for s in scratch],
        cost_estimate=pl.CostEstimate(flops=flops, bytes_accessed=0, transcendentals=0),
        compiler_params=pltpu.CompilerParams(vmem_limit_bytes=VMEM_LIMIT),
        name=kernel.__name__,
    )(*args)


def neighbours(far, near):
    count = lax.axis_size("region")
    mate = [(r, r ^ 1) for r in range(count)]
    cross = [(r, (r + 1) % count if r % 2 else (r - 1) % count) for r in range(count)]
    return lax.ppermute(far, "region", cross), lax.ppermute(near, "region", mate)


def over_slots(msg):
    count = lax.axis_size("slot")
    if count == 2:
        return lax.ppermute(msg, "slot", [(0, 1), (1, 0)])
    mine = msg.astype(F32)
    return (lax.psum(mine, "slot") - mine).astype(BF16)


def shards(ensemble, observations, operator_weight, obs_precision, channel_mask):
    slots, patches, rows, members = ensemble.shape
    channels = operator_weight.shape[0]
    if lax.axis_size("region") % 2 or patches % 2 or not 4 <= patches <= 16:
        raise ValueError("unsupported split")
    inner = patches - 2
    odd = (lax.axis_index("region") % 2).astype(jnp.int32).reshape(1)
    edge = ((members + 16, members), BF16)
    gram = lambda n: ((n, members, members), F32)
    grad = lambda n: ((n, members), F32)
    message = lambda n: ((n // 2 * members + -(-(n // 2 + n) // 16) * 16, members), BF16)
    inner_out = [gram(inner), grad(inner), message(inner), gram(2), grad(2)]
    inner_scratch = (
        ((inner, rows, slots * members), BF16),
        [((inner, slots * channels, members), BF16), ((inner, members, slots * channels), BF16)],
        gram(inner),
    )
    scratch = lambda n: (
        ((n, rows, slots * members), BF16),
        [((n, slots * channels, members), BF16), ((n, members, slots * channels), BF16)],
    )
    rw = ((slots, channels, members), F32)
    ow = ((16, slots * channels), BF16)
    state = lambda n: ((slots, n, rows, members), BF16)
    prec = obs_precision[None, :]
    dma = pltpu.SemaphoreType.DMA
    hbm = lambda x: pltpu.with_memory_space_constraint(x, pltpu.HBM)

    states, weight, qe, qge, far, near, root_w, obs_w = call(
        first_kernel,
        [state(patches), (operator_weight.shape, BF16), gram(2), grad(2), edge, edge, rw, ow],
        (odd, hbm(ensemble), hbm(operator_weight), hbm(observations), hbm(prec), hbm(channel_mask)),
        "shhhhh",
        scratch(2) + (
            (observations.shape, F32),
            (prec.shape, F32),
            (channel_mask.shape, jnp.int32),
            dma((4 + slots * patches,)),
        ),
    )
    far, near = neighbours(far, near)
    *loc, msg, qi, qgi = call(
        inner_kernel, inner_out, (states, weight, root_w, obs_w, qe, qge), "vvvvvv", inner_scratch
    )
    parts = (states,)
    for step in range(OUTER):
        sums = tuple(
            call(sums_kernel, [gram(inner), grad(inner), grad(inner)], (*loc, over_slots(msg)), "vvv", flops=10 ** 8)
        )
        *loc, msg = call(
            combine_kernel,
            [gram(2), grad(2), message(2)],
            (odd, qe, qge, qi, qgi, far, near),
            "svvvvvv",
        )
        sums += (*loc, over_slots(msg))
        if step == OUTER - 1:
            break
        if len(parts) > 1:
            edges, inside = parts
            states = jnp.concatenate([edges[:, :1], inside, edges[:, 1:]], axis=1)
        mix, edges, qe, qge, far, near = call(
            root_kernel,
            [((inner, members, members), BF16), state(2), gram(2), grad(2), edge, edge],
            (odd, *sums, states, weight, root_w, obs_w),
            "s" + "v" * 10,
            scratch(2),
        )
        far, near = neighbours(far, near)
        inside, *loc, msg, qi, qgi = call(
            advance_kernel,
            [state(inner)] + inner_out,
            (mix, states, weight, root_w, obs_w, qe, qge),
            "vvvvvvv",
            inner_scratch,
        )
        parts = (edges, inside)
    return call(
        last_kernel,
        [state(patches)],
        sums + parts,
        "v" * (6 + len(parts)),
        (state(patches), dma((slots * patches,))),
        out_kinds="h",
    )[0]


def solution(mesh):
    return jax.shard_map(
        shards,
        mesh=mesh,
        in_specs=(
            P("slot", "region", None, None),
            P("slot", "region", None),
            P(),
            P(),
            P("slot", None),
        ),
        out_specs=P("slot", "region", None, None),
        check_vma=False,
    )
```
